512 devices in a mesh: chan: 8 (over z), seq: 64 (over y, x, core).
Axes of the slice: x: 4, y: 8, z: 8, core: 2. Of those that a mesh axis runs over, the one named last changes fastest.
Arguments:
- inputs: bfloat16 [3, 8192, 2, 4096], P(None, 'seq', None, 'chan'), may hold values from -6 to 6
- decay_rate: float32 [4096], P('chan'), may hold values from 6.1035156e-05 to 0.03
- phase: float32 [4096], P('chan'), may hold values from -3.140625 to 3.140625
- keep: float32 [3, 8192], replicated, may hold values from 0.5 to 1
Outputs:
- states: bfloat16 [3, 8192, 2, 4096], P(None, 'seq', None, 'chan')
The draws below stay inside these ranges and needn't reach their ends.
All inputs are finite; a program needn't handle non-finite values.
Results may differ from the reference program's by a relative error of at most 0.001.
Values sent between devices are 32-bit elements; how exact they have to be, the bound alone decides.
No kernel may reach another device: no remote copies, remote signals or barrier semaphores. Data moves between devices by JAX's collectives and lax.ppermute only.
A program may use at most 64 MiB of HBM per device.

```python
import math
import jax
import jax.numpy as jnp
from jax import lax

CHANNELS = 4096
SEQS = 3
SEQ_LEN = 8192


def draw_keep(key, part):
    first_key, second_key = jax.random.split(jax.random.fold_in(key, 11))
    spots = jax.random.randint(first_key, (SEQS, 8), 0, SEQ_LEN)
    levels = jax.random.uniform(second_key, (SEQS, 8), jnp.float32, 0.5, 0.8)
    row_ids = jnp.broadcast_to(jnp.arange(SEQS)[:, None], (SEQS, 8))
    return jnp.ones((SEQS, SEQ_LEN), jnp.float32).at[row_ids, spots].set(levels)


def steps_of(rng, dims, pieces, least, top_value):
    def one(axis_at, blocks):
        steps = jax.random.uniform(jax.random.fold_in(jax.random.fold_in(rng, 6), axis_at), (blocks,), jnp.float32, least / len(pieces), top_value / len(pieces))
        return jnp.repeat(jnp.exp(steps), dims[axis_at] // blocks).reshape((-1,) + (1,) * (len(dims) - axis_at - 1))

    gain = one(*pieces[0])
    for cut in pieces[1:]:
        gain = gain * one(*cut)
    return gain


def normal_values(key, dims, width, bound, cuts=(), kind=jnp.bfloat16):
    values = width * jax.random.normal(key, dims, jnp.float32)
    if cuts:
        values = values * steps_of(key, dims, cuts, -0.22, 0.18)
    return jnp.clip(values, -bound, bound).astype(kind)


def setup_inputs(seed: int = 0) -> dict:
    streams_of = jax.random.split(jax.random.key(seed), 5)
    inputs = normal_values(streams_of[0], (SEQS, SEQ_LEN, 2, CHANNELS), 1.0, 6.0, ((1, 64), (3, 8)))
    decay_rate = jnp.clip(jnp.exp(math.log(0.03) - 6.1975026 * jax.random.uniform(streams_of[1], (CHANNELS,), jnp.float32) ** steps_of(streams_of[1], (CHANNELS,), ((0, 8),), -0.2, 0.2)), 6.103515625e-05, 0.03)
    phase = jnp.clip(jax.random.uniform(streams_of[2], (CHANNELS,), jnp.float32, -3.140625, 3.140625), -3.140625, 3.140625)
    keep = draw_keep(jax.random.fold_in(streams_of[4], 71), 0)
    return {"inputs": inputs, "decay_rate": decay_rate, "phase": phase, "keep": keep}


def reference(inputs, decay_rate, phase, keep):
    magnitude = jnp.exp(-decay_rate)
    lam_re = magnitude * jnp.cos(phase)
    lam_im = magnitude * jnp.sin(phase)
    gamma = jnp.sqrt(-jnp.expm1(-2.0 * decay_rate))

    def advance(carry, items):
        state_re, state_im = carry
        factor, source_re, source_im = items
        dec_re = factor * lam_re
        dec_im = factor * lam_im
        next_re = dec_re * state_re - dec_im * state_im + source_re
        next_im = dec_re * state_im + dec_im * state_re + source_im
        return ((next_re, next_im), (next_re, next_im))

    def one_sequence(pair):
        sequence, factors = pair
        drive_re = sequence[:, 0, :].astype(jnp.float32) * gamma[None, :]
        drive_im = sequence[:, 1, :].astype(jnp.float32) * gamma[None, :]
        start = (jnp.zeros_like(lam_re), jnp.zeros_like(lam_re))
        _, (all_re, all_im) = lax.scan(advance, start, (factors, drive_re, drive_im))
        return jnp.stack([all_re, all_im], axis=1).astype(jnp.bfloat16)
    return lax.map(one_sequence, (inputs, keep))
```

```python
import functools

import jax
import jax.numpy as jnp
from jax import lax
from jax.experimental import pallas as pl
from jax.experimental.pallas import tpu as pltpu
from jax.sharding import Mesh
from jax.sharding import PartitionSpec as P

LANES = 128
ROWS = 8
STEP = 16
GROUP = 8

HBM = pl.BlockSpec(memory_space=pltpu.HBM)
VMEM = pl.BlockSpec(memory_space=pltpu.VMEM)


def times(one, two):
    a, b = one
    c, d = two
    return (a * c - b * d, a * d + b * c)


def powers(base, count):
    found = [None, base]
    for n in range(2, count):
        found.append(times(found[n // 2], found[n - n // 2]))
    return found


def parity():
    return lax.broadcasted_iota(jnp.int32, (ROWS, LANES), 0) % 2 == 0


def turned(value, even):
    return jnp.where(even, -pltpu.roll(value, ROWS - 1, 0), pltpu.roll(value, 1, 0))


def doubled(rows):
    return jnp.concatenate([rows[j // 2 : j // 2 + 1] for j in range(ROWS)], axis=0)


def lane_product(value):
    for width, turns in ((1, 4), (4, 4), (16, 4), (64, 2)):
        rolled = [value] + [pltpu.roll(value, width * n, 1) for n in range(1, turns)]
        while len(rolled) > 1:
            rolled = [rolled[n] * rolled[n + 1] for n in range(0, len(rolled), 2)]
        value = rolled[0]
    return value


def minus_expm1_twice(rate):
    u = 2.0 * rate
    series = u * (1.0 - u / 2 * (1.0 - u / 3 * (1.0 - u / 4 * (1.0 - u / 5 * (1.0 - u / 6)))))
    return jnp.where(u < 0.1, series, 1.0 - jnp.exp(-u))


def first(batch, length, x_hbm, rate_hbm, phase_hbm, keep_hbm, x_ref, send_ref, start_ref, chunk_ref,
          block_ref, row_ref, small_ref, factor_ref, reach_ref, keep_ref, param_ref, own_ref, keep_all, sems):
    row, col = lax.axis_index("row"), lax.axis_index("col")
    chunks = length // STEP
    span = length * ROWS
    loads = [
        pltpu.make_async_copy(rate_hbm, param_ref.at[0], sems.at[0]),
        pltpu.make_async_copy(phase_hbm, param_ref.at[1], sems.at[1]),
        pltpu.make_async_copy(keep_hbm.at[row * GROUP + col], own_ref, sems.at[2]),
        pltpu.make_async_copy(keep_hbm, keep_all, sems.at[3]),
    ] + [
        pltpu.make_async_copy(x_hbm.at[pl.ds(s * span, span)], x_ref.at[pl.ds(s * span, span)], sems.at[4 + s])
        for s in range(batch)
    ]
    for load in loads:
        load.start()
    even = parity()
    loads[0].wait()
    loads[1].wait()
    rate, phase = doubled(param_ref[0]), doubled(param_ref[1])
    magnitude = jnp.exp(-rate)
    one = jnp.ones_like(rate)
    zero = jnp.zeros_like(rate)
    lam = (magnitude * jnp.cos(phase), magnitude * jnp.sin(phase))
    step = powers(lam, STEP + 1)
    chunk = powers(step[STEP], chunks + 1)
    block = powers(chunk[chunks], GROUP + 1)
    line = powers(block[GROUP], GROUP)
    small_ref[0], small_ref[1] = lam
    small_ref[2] = jnp.sqrt(minus_expm1_twice(rate))
    for ref, found, before in ((chunk_ref, chunk[:chunks], 0), (block_ref, block[:GROUP], GROUP), (row_ref, line, GROUP)):
        for part in range(2):
            for n in range(before):
                ref[part, n] = zero
            ref[part, before] = zero if part else one
            for n in range(1, len(found)):
                ref[part, before + n] = found[n][part]
    loads[3].wait()
    products = [lane_product(keep_all[row * GROUP + m]) for m in range(GROUP)]
    for line_at in range(GROUP):
        product = keep_all[line_at * GROUP]
        for m in range(1, GROUP):
            product = product * keep_all[line_at * GROUP + m]
        products.append(lane_product(product))
    for n, product in enumerate(products):
        for s in range(batch):
            factor_ref[n, s] = jnp.broadcast_to(product[s : s + 1], (ROWS, LANES))
    loads[2].wait()
    for s in range(batch):
        loads[4 + s].wait()
        direct, cross, decay = [None] * chunks, [None] * chunks, [None] * chunks
        for i in range(STEP):
            for k in range(chunks):
                t = k * STEP + i
                x = x_ref[pl.ds(s * span + t * ROWS, ROWS)].astype(jnp.float32)
                kept = jnp.full((ROWS, LANES), own_ref[s, t], jnp.float32)
                keep_ref[pl.ds(s * length + t, 1)] = kept[:1]
                n = STEP - 1 - i
                dir_x, cross_x = (x, None) if n == 0 else (step[n][0] * x, step[n][1] * x)
                if i == 0:
                    direct[k], cross[k], decay[k] = dir_x, cross_x, kept
                else:
                    direct[k] = kept * direct[k] + dir_x
                    cross[k] = kept * cross[k] if cross_x is None else kept * cross[k] + cross_x
                    decay[k] = kept * decay[k]
        state, reach = zero, one
        for k in range(chunks):
            start_ref[s, k] = state
            reach_ref[pl.ds(s * chunks + k, 1)] = reach[:1]
            end = direct[k] + turned(cross[k], even)
            if k:
                end = decay[k] * (step[STEP][0] * state + step[STEP][1] * turned(state, even)) + end
            state, reach = end, reach * decay[k]
        for n in range(GROUP):
            send_ref[n, s] = state


def second(batch, got_ref, block_ref, factor_ref, send_ref):
    even = parity()
    for s in range(batch):
        direct = cross = None
        for m in range(GROUP):
            x = got_ref[m, s]
            a, b = block_ref[0, 2 * GROUP - 1 - m], block_ref[1, 2 * GROUP - 1 - m]
            if m == 0:
                direct, cross = a * x, b * x
            else:
                direct = factor_ref[m, s] * direct + a * x
                cross = factor_ref[m, s] * cross + b * x
        total = direct + turned(cross, even)
        for n in range(GROUP):
            send_ref[n, s] = total


def before_me(me, got_ref, power_ref, factor_ref, at, s, even):
    direct = cross = jnp.zeros((ROWS, LANES), jnp.float32)
    reach = jnp.ones((ROWS, LANES), jnp.float32)
    for m in range(GROUP):
        n = GROUP - 1 + me - m
        kept = jnp.where(m < me, factor_ref[at + m, s], 1.0)
        direct = kept * direct + power_ref[0, n] * got_ref[m, s]
        cross = kept * cross + power_ref[1, n] * got_ref[m, s]
        reach = kept * reach
    return direct + turned(cross, even), reach


def third(batch, length, x_ref, near_ref, far_ref, start_ref, chunk_ref, block_ref, row_ref, small_ref,
          factor_ref, reach_ref, keep_ref, y_hbm, y_ref, sems):
    row, col = lax.axis_index("row"), lax.axis_index("col")
    chunks = length // STEP
    span = length * ROWS
    even = parity()
    carries = []
    for s in range(batch):
        inside, reach = before_me(col, near_ref, block_ref, factor_ref, 0, s, even)
        lines, _ = before_me(row, far_ref, row_ref, factor_ref, GROUP, s, even)
        a, b = block_ref[0, GROUP + col], block_ref[1, GROUP + col]
        carries.append(reach * (a * lines + b * turned(lines, even)) + inside)
    lam_re, gamma = small_ref[0], small_ref[2]
    lam_im = jnp.where(even, -small_ref[1], small_ref[1])
    stores = []
    for s in range(batch):
        carry, spun = carries[s], turned(carries[s], even)
        state = [
            start_ref[s, k]
            + jnp.broadcast_to(reach_ref[pl.ds(s * chunks + k, 1)], (ROWS, LANES))
            * (chunk_ref[0, k] * carry + chunk_ref[1, k] * spun)
            for k in range(chunks)
        ]
        for i in range(STEP):
            for k in range(chunks):
                t = k * STEP + i
                h = state[k]
                swapped = jnp.where(even, pltpu.roll(h, ROWS - 1, 0), pltpu.roll(h, 1, 0))
                kept = jnp.broadcast_to(keep_ref[pl.ds(s * length + t, 1)], (ROWS, LANES))
                x = x_ref[pl.ds(s * span + t * ROWS, ROWS)].astype(jnp.float32)
                state[k] = kept * (lam_re * h + lam_im * swapped) + x
                y_ref[pl.ds(s * span + t * ROWS, ROWS)] = (gamma * state[k]).astype(jnp.bfloat16)
        store = pltpu.make_async_copy(y_ref.at[pl.ds(s * span, span)], y_hbm.at[pl.ds(s * span, span)], sems.at[s])
        store.start()
        stores.append(store)
    for store in stores:
        store.wait()


def shards(inputs, decay_rate, phase, keep):
    batch, length, parts, width = inputs.shape
    tiles = width // LANES
    blocks = keep.shape[1] // length
    chunks = length // STEP
    f32 = functools.partial(jax.ShapeDtypeStruct, dtype=jnp.float32)
    total = batch * length * ROWS
    x = inputs.reshape(batch, length, parts, tiles, LANES).transpose(0, 1, 3, 2, 4).reshape(total, LANES)
    kept = keep.reshape(batch, blocks, length).transpose(1, 0, 2)
    exchange = f32((GROUP, batch, ROWS, LANES))
    x, send, start, chunk, block, line, small, factor, reach, keeps = pl.pallas_call(
        functools.partial(first, batch, length),
        out_shape=[
            jax.ShapeDtypeStruct((total, LANES), jnp.bfloat16),
            exchange,
            f32((batch, chunks, ROWS, LANES)),
            f32((2, chunks, ROWS, LANES)),
            f32((2, 2 * GROUP, ROWS, LANES)),
            f32((2, 2 * GROUP, ROWS, LANES)),
            f32((3, ROWS, LANES)),
            f32((2 * GROUP, batch, ROWS, LANES)),
            f32((batch * chunks, LANES)),
            f32((batch * length, LANES)),
        ],
        in_specs=[HBM] * 4,
        out_specs=[VMEM] * 10,
        scratch_shapes=[
            pltpu.VMEM((2, tiles, LANES), jnp.float32),
            pltpu.SMEM((batch, LANES), jnp.float32),
            pltpu.VMEM((blocks, batch, LANES), jnp.float32),
            pltpu.SemaphoreType.DMA((4 + batch,)),
        ],
    )(x, decay_rate.reshape(tiles, LANES), phase.reshape(tiles, LANES), kept)

    def swap(value, axis):
        flat = value.reshape(GROUP, batch * ROWS, LANES)
        return lax.all_to_all(flat, axis, 0, 0, tiled=True).reshape(value.shape)

    near = swap(send, "col")
    totals = pl.pallas_call(
        functools.partial(second, batch),
        out_shape=exchange,
        in_specs=[VMEM] * 3,
        out_specs=VMEM,
    )(near, block, factor)
    far = swap(totals, "row")
    y = pl.pallas_call(
        functools.partial(third, batch, length),
        out_shape=jax.ShapeDtypeStruct((total, LANES), jnp.bfloat16),
        in_specs=[VMEM] * 11,
        out_specs=HBM,
        scratch_shapes=[
            pltpu.VMEM((total, LANES), jnp.bfloat16),
            pltpu.SemaphoreType.DMA((batch,)),
        ],
    )(x, near, far, start, chunk, block, line, small, factor, reach, keeps)
    y = y.reshape(batch, length, tiles, parts, LANES).transpose(0, 1, 3, 2, 4)
    return y.reshape(inputs.shape)


def solution(mesh):
    split = Mesh(mesh.devices.reshape(mesh.shape["chan"], GROUP, GROUP), ("chan", "row", "col"))
    seq = ("row", "col")
    return jax.shard_map(
        shards,
        mesh=split,
        in_specs=(P(None, seq, None, "chan"), P("chan"), P("chan"), P()),
        out_specs=P(None, seq, None, "chan"),
        check_vma=False,
    )
```

```python
import functools

import jax
import jax.numpy as jnp
from jax import lax
from jax.experimental import pallas as pl
from jax.experimental.pallas import tpu as pltpu
from jax.sharding import Mesh
from jax.sharding import PartitionSpec as P

LANES = 128
ROWS = 8
LIMIT = pltpu.CompilerParams(vmem_limit_bytes=8388608)
STEP = 16
GROUP = 8

HBM = pl.BlockSpec(memory_space=pltpu.HBM)
VMEM = pl.BlockSpec(memory_space=pltpu.VMEM)


def times(one, two):
    a, b = one
    c, d = two
    return (a * c - b * d, a * d + b * c)


def powers(base, count):
    found = [None, base]
    for n in range(2, count):
        found.append(times(found[n // 2], found[n - n // 2]))
    return found


def parity():
    return lax.broadcasted_iota(jnp.int32, (ROWS, LANES), 0) % 2 == 0


def turned(value, even):
    return jnp.where(even, -pltpu.roll(value, ROWS - 1, 0), pltpu.roll(value, 1, 0))


def doubled(rows):
    return jnp.concatenate([rows[j // 2 : j // 2 + 1] for j in range(ROWS)], axis=0)


def lane_product(value):
    for width, turns in ((1, 4), (4, 4), (16, 4), (64, 2)):
        rolled = [value] + [pltpu.roll(value, width * n, 1) for n in range(1, turns)]
        while len(rolled) > 1:
            rolled = [rolled[n] * rolled[n + 1] for n in range(0, len(rolled), 2)]
        value = rolled[0]
    return value


def minus_expm1_twice(rate):
    u = 2.0 * rate
    series = u * (1.0 - u / 2 * (1.0 - u / 3 * (1.0 - u / 4 * (1.0 - u / 5 * (1.0 - u / 6)))))
    return jnp.where(u < 0.1, series, 1.0 - jnp.exp(-u))


def first(batch, length, x_hbm, rate_hbm, phase_hbm, keep_hbm, x_ref, send_ref, start_ref, chunk_ref,
          block_ref, row_ref, small_ref, factor_ref, reach_ref, keep_ref, param_ref, own_ref, keep_all, sems):
    row, col = lax.axis_index("row"), lax.axis_index("col")
    chunks = length // STEP
    span = length * ROWS
    loads = [
        pltpu.make_async_copy(rate_hbm, param_ref.at[0], sems.at[0]),
        pltpu.make_async_copy(phase_hbm, param_ref.at[1], sems.at[1]),
        pltpu.make_async_copy(keep_hbm.at[row * GROUP + col], own_ref, sems.at[2]),
        pltpu.make_async_copy(keep_hbm, keep_all, sems.at[3]),
    ] + [
        pltpu.make_async_copy(x_hbm.at[pl.ds(s * span, span)], x_ref.at[pl.ds(s * span, span)], sems.at[4 + s])
        for s in range(batch)
    ]
    for load in loads:
        load.start()
    even = parity()
    loads[0].wait()
    loads[1].wait()
    rate, phase = doubled(param_ref[0]), doubled(param_ref[1])
    magnitude = jnp.exp(-rate)
    one = jnp.ones_like(rate)
    zero = jnp.zeros_like(rate)
    lam = (magnitude * jnp.cos(phase), magnitude * jnp.sin(phase))
    step = powers(lam, STEP + 1)
    chunk = powers(step[STEP], chunks + 1)
    block = powers(chunk[chunks], GROUP + 1)
    line = powers(block[GROUP], GROUP)
    small_ref[0], small_ref[1] = lam
    small_ref[2] = jnp.sqrt(minus_expm1_twice(rate))
    for ref, found, before in ((chunk_ref, chunk[:chunks], 0), (block_ref, block[:GROUP], GROUP), (row_ref, line, GROUP)):
        for part in range(2):
            for n in range(before):
                ref[part, n] = zero
            ref[part, before] = zero if part else one
            for n in range(1, len(found)):
                ref[part, before + n] = found[n][part]
    loads[3].wait()
    products = [lane_product(keep_all[row * GROUP + m]) for m in range(GROUP)]
    for line_at in range(GROUP):
        product = keep_all[line_at * GROUP]
        for m in range(1, GROUP):
            product = product * keep_all[line_at * GROUP + m]
        products.append(lane_product(product))
    for n, product in enumerate(products):
        for s in range(batch):
            factor_ref[n, s] = jnp.broadcast_to(product[s : s + 1], (ROWS, LANES))
    loads[2].wait()
    for s in range(batch):
        loads[4 + s].wait()
        direct, cross, decay = [None] * chunks, [None] * chunks, [None] * chunks
        for i in range(STEP):
            for k in range(chunks):
                t = k * STEP + i
                x = x_ref[pl.ds(s * span + t * ROWS, ROWS)].astype(jnp.float32)
                kept = jnp.full((ROWS, LANES), own_ref[s, t], jnp.float32)
                keep_ref[pl.ds(s * length + t, 1)] = kept[:1]
                n = STEP - 1 - i
                dir_x, cross_x = (x, None) if n == 0 else (step[n][0] * x, step[n][1] * x)
                if i == 0:
                    direct[k], cross[k], decay[k] = dir_x, cross_x, kept
                else:
                    direct[k] = kept * direct[k] + dir_x
                    cross[k] = kept * cross[k] if cross_x is None else kept * cross[k] + cross_x
                    decay[k] = kept * decay[k]
        state, reach = zero, one
        for k in range(chunks):
            start_ref[s, k] = state
            reach_ref[pl.ds(s * chunks + k, 1)] = reach[:1]
            end = direct[k] + turned(cross[k], even)
            if k:
                end = decay[k] * (step[STEP][0] * state + step[STEP][1] * turned(state, even)) + end
            state, reach = end, reach * decay[k]
        for n in range(GROUP):
            send_ref[n, s] = state


def second(batch, got_ref, block_ref, factor_ref, send_ref):
    even = parity()
    for s in range(batch):
        direct = cross = None
        for m in range(GROUP):
            x = got_ref[m, s]
            a, b = block_ref[0, 2 * GROUP - 1 - m], block_ref[1, 2 * GROUP - 1 - m]
            if m == 0:
                direct, cross = a * x, b * x
            else:
                direct = factor_ref[m, s] * direct + a * x
                cross = factor_ref[m, s] * cross + b * x
        total = direct + turned(cross, even)
        for n in range(GROUP):
            send_ref[n, s] = total


def before_me(me, got_ref, power_ref, factor_ref, at, s, even):
    direct = cross = jnp.zeros((ROWS, LANES), jnp.float32)
    reach = jnp.ones((ROWS, LANES), jnp.float32)
    for m in range(GROUP):
        n = GROUP - 1 + me - m
        kept = jnp.where(m < me, factor_ref[at + m, s], 1.0)
        direct = kept * direct + power_ref[0, n] * got_ref[m, s]
        cross = kept * cross + power_ref[1, n] * got_ref[m, s]
        reach = kept * reach
    return direct + turned(cross, even), reach


def third(batch, length, x_ref, near_ref, far_ref, start_ref, chunk_ref, block_ref, row_ref, small_ref,
          factor_ref, reach_ref, keep_ref, y_hbm, y_ref, sems):
    row, col = lax.axis_index("row"), lax.axis_index("col")
    chunks = length // STEP
    span = length * ROWS
    even = parity()
    carries = []
    for s in range(batch):
        inside, reach = before_me(col, near_ref, block_ref, factor_ref, 0, s, even)
        lines, _ = before_me(row, far_ref, row_ref, factor_ref, GROUP, s, even)
        a, b = block_ref[0, GROUP + col], block_ref[1, GROUP + col]
        carries.append(reach * (a * lines + b * turned(lines, even)) + inside)
    lam_re, gamma = small_ref[0], small_ref[2]
    lam_im = jnp.where(even, -small_ref[1], small_ref[1])
    stores = []
    for s in range(batch):
        carry, spun = carries[s], turned(carries[s], even)
        state = [
            start_ref[s, k]
            + jnp.broadcast_to(reach_ref[pl.ds(s * chunks + k, 1)], (ROWS, LANES))
            * (chunk_ref[0, k] * carry + chunk_ref[1, k] * spun)
            for k in range(chunks)
        ]
        for i in range(STEP):
            for k in range(chunks):
                t = k * STEP + i
                h = state[k]
                swapped = jnp.where(even, pltpu.roll(h, ROWS - 1, 0), pltpu.roll(h, 1, 0))
                kept = jnp.broadcast_to(keep_ref[pl.ds(s * length + t, 1)], (ROWS, LANES))
                x = x_ref[pl.ds(s * span + t * ROWS, ROWS)].astype(jnp.float32)
                state[k] = kept * (lam_re * h + lam_im * swapped) + x
                y_ref[pl.ds(s * span + t * ROWS, ROWS)] = (gamma * state[k]).astype(jnp.bfloat16)
        store = pltpu.make_async_copy(y_ref.at[pl.ds(s * span, span)], y_hbm.at[pl.ds(s * span, span)], sems.at[s])
        store.start()
        stores.append(store)
    for store in stores:
        store.wait()


def shards(inputs, decay_rate, phase, keep):
    batch, length, parts, width = inputs.shape
    tiles = width // LANES
    blocks = keep.shape[1] // length
    chunks = length // STEP
    f32 = functools.partial(jax.ShapeDtypeStruct, dtype=jnp.float32)
    total = batch * length * ROWS
    x = inputs.reshape(batch, length, parts, tiles, LANES).transpose(0, 1, 3, 2, 4).reshape(total, LANES)
    kept = keep.reshape(batch, blocks, length).transpose(1, 0, 2)
    exchange = f32((GROUP, batch, ROWS, LANES))
    x, send, start, chunk, block, line, small, factor, reach, keeps = pl.pallas_call(
        functools.partial(first, batch, length),
        out_shape=[
            jax.ShapeDtypeStruct((total, LANES), jnp.bfloat16),
            exchange,
            f32((batch, chunks, ROWS, LANES)),
            f32((2, chunks, ROWS, LANES)),
            f32((2, 2 * GROUP, ROWS, LANES)),
            f32((2, 2 * GROUP, ROWS, LANES)),
            f32((3, ROWS, LANES)),
            f32((2 * GROUP, batch, ROWS, LANES)),
            f32((batch * chunks, LANES)),
            f32((batch * length, LANES)),
        ],
        compiler_params=LIMIT,
        in_specs=[HBM] * 4,
        out_specs=[VMEM] * 10,
        scratch_shapes=[
            pltpu.VMEM((2, tiles, LANES), jnp.float32),
            pltpu.SMEM((batch, LANES), jnp.float32),
            pltpu.VMEM((blocks, batch, LANES), jnp.float32),
            pltpu.SemaphoreType.DMA((4 + batch,)),
        ],
    )(*(pltpu.with_memory_space_constraint(v, pltpu.HBM) for v in (x, decay_rate.reshape(tiles, LANES), phase.reshape(tiles, LANES), kept)))

    def swap(value, axis):
        flat = value.reshape(GROUP, batch * ROWS, LANES)
        return lax.all_to_all(flat, axis, 0, 0, tiled=True).reshape(value.shape)

    near = swap(send, "col")
    totals = pl.pallas_call(
        functools.partial(second, batch),
        out_shape=exchange,
        compiler_params=LIMIT,
        in_specs=[VMEM] * 3,
        out_specs=VMEM,
    )(near, block, factor)
    far = swap(totals, "row")
    y = pl.pallas_call(
        functools.partial(third, batch, length),
        out_shape=jax.ShapeDtypeStruct((total, LANES), jnp.bfloat16),
        compiler_params=LIMIT,
        in_specs=[VMEM] * 11,
        out_specs=HBM,
        scratch_shapes=[
            pltpu.VMEM((total, LANES), jnp.bfloat16),
            pltpu.SemaphoreType.DMA((batch,)),
        ],
    )(x, near, far, start, chunk, block, line, small, factor, reach, keeps)
    y = y.reshape(batch, length, tiles, parts, LANES).transpose(0, 1, 3, 2, 4)
    return y.reshape(inputs.shape)


def solution(mesh):
    split = Mesh(mesh.devices.reshape(mesh.shape["chan"], GROUP, GROUP), ("chan", "row", "col"))
    seq = ("row", "col")
    return jax.shard_map(
        shards,
        mesh=split,
        in_specs=(P(None, seq, None, "chan"), P("chan"), P("chan"), P()),
        out_specs=P(None, seq, None, "chan"),
        check_vma=False,
    )
```

```python
import functools

import jax
import jax.numpy as jnp
from jax import lax
from jax.experimental import pallas as pl
from jax.experimental.pallas import tpu as pltpu
from jax.sharding import Mesh
from jax.sharding import PartitionSpec as P

LANES = 128
ROWS = 8
STEP = 16
NEAR = 16
FAR = 4
WIDE = 8
SENDS = (
    ((0, 1, 0),),
    ((0, 3, 0),),
    ((0, 2, 1), (1, 3, 1)),
    ((1, 2, 0), (2, 3, 0)),
)

HBM = pl.BlockSpec(memory_space=pltpu.HBM)
VMEM = pl.BlockSpec(memory_space=pltpu.VMEM)
LIMIT = pltpu.CompilerParams(vmem_limit_bytes=8 * 1024 * 1024)


def times(one, two):
    a, b = one
    c, d = two
    return (a * c - b * d, a * d + b * c)


def powers(base, count):
    found = [None, base]
    for n in range(2, count):
        found.append(times(found[n // 2], found[n - n // 2]))
    return found


def places():
    return lax.broadcasted_iota(jnp.int32, (ROWS, LANES), 0)


def sign():
    return jnp.where(places() % 2 == 0, -1.0, 1.0)


def swapped(value):
    return jnp.take_along_axis(value, places() ^ 1, axis=0, mode="promise_in_bounds")


def spread(row):
    return jnp.broadcast_to(row, (ROWS, LANES))


def doubled(rows):
    return jnp.concatenate([rows[j // 2 : j // 2 + 1] for j in range(ROWS)], axis=0)


def lane_product(value):
    for width, turns in ((1, 4), (4, 4), (16, 4), (64, 2)):
        rolled = [value] + [pltpu.roll(value, width * n, 1) for n in range(1, turns)]
        while len(rolled) > 1:
            rolled = [rolled[n] * rolled[n + 1] for n in range(0, len(rolled), 2)]
        value = rolled[0]
    return value


def minus_expm1_twice(rate):
    u = 2.0 * rate
    series = u * (1.0 - u / 2 * (1.0 - u / 3 * (1.0 - u / 4 * (1.0 - u / 5 * (1.0 - u / 6)))))
    return jnp.where(u < 0.1, series, 1.0 - jnp.exp(-u))


def first(batch, length, x_hbm, rate_hbm, phase_hbm, keep_hbm, local_ref, send_ref, start_ref, chunk_ref, step_ref,
          reach_ref, decay_ref, total_ref, inside_ref, lines_ref, x_ref, keep_ref, param_ref, own_ref, block_ref,
          run_ref, sems):
    me = lax.axis_index("seq")
    run, at = me // NEAR, me % NEAR
    chunks = length // STEP
    span = length * ROWS
    pieces = [
        pltpu.make_async_copy(x_hbm.at[pl.ds(s * span, span)], x_ref.at[pl.ds(s * span, span)], sems.at[4 + s])
        for s in range(batch)
    ]
    loads = [
        pltpu.make_async_copy(rate_hbm, param_ref.at[0], sems.at[0]),
        pltpu.make_async_copy(phase_hbm, param_ref.at[1], sems.at[1]),
        pltpu.make_async_copy(keep_hbm.at[me], own_ref, sems.at[2]),
        pltpu.make_async_copy(keep_hbm, keep_ref, sems.at[3]),
    ]
    for load in loads[:3] + pieces[:1] + loads[3:] + pieces[1:]:
        load.start()
    flip = sign()
    loads[0].wait()
    loads[1].wait()
    rate, phase = doubled(param_ref[0]), doubled(param_ref[1])
    magnitude = jnp.exp(-rate)
    one, zero = jnp.ones_like(rate), jnp.zeros_like(rate)
    lam = (magnitude * jnp.cos(phase), magnitude * jnp.sin(phase))
    gamma = jnp.sqrt(minus_expm1_twice(rate))
    step = powers(lam, STEP + 1)
    chunk = powers(step[STEP], chunks + 1)
    block = powers(chunk[chunks], NEAR + 1)
    run_ref[0], run_ref[1] = block[NEAR]
    for part in range(2):
        for n in range(STEP):
            step_ref[part, n] = step[n + 1][part]
        for n in range(NEAR):
            block_ref[part, n] = zero
        block_ref[part, NEAR] = zero if part else one
        for n in range(1, NEAR):
            block_ref[part, NEAR + n] = block[n][part]
        chunk_ref[part, 0] = zero if part else one
        for n in range(1, chunks):
            chunk_ref[part, n] = chunk[n][part]
    lam_re, lam_im = lam[0], lam[1] * flip
    jump_re, jump_im = step[STEP][0], step[STEP][1] * flip

    def scan(s):
        state, decay = [None] * chunks, [None] * chunks
        for i in range(STEP):
            for k in range(chunks):
                t = k * STEP + i
                x = gamma * x_ref[pl.ds(s * span + t * ROWS, ROWS)].astype(jnp.float32)
                kept = jnp.full((ROWS, LANES), own_ref[s, t], jnp.float32)
                if i == 0:
                    state[k], decay[k] = x, kept
                else:
                    h = state[k]
                    state[k] = kept * (lam_re * h + lam_im * swapped(h)) + x
                    decay[k] = kept * decay[k]
                local_ref[s, t] = state[k]
                decay_ref[pl.ds(s * length + t, 1)] = decay[k][:1]
        return state, decay

    def chain(s, ends, decays):
        state, reach = zero, one
        for k in range(chunks):
            start_ref[s, k] = state
            reach_ref[pl.ds(s * chunks + k, 1)] = reach[:1]
            if k:
                state = decays[k] * (jump_re * state + jump_im * swapped(state)) + ends[k]
            else:
                state = ends[k]
            reach = reach * decays[k]
        for n in range(NEAR):
            send_ref[n, s] = state

    def block_products():
        near = [lane_product(keep_ref[run * NEAR + m]) for m in range(NEAR)]
        far = []
        for n in range(FAR):
            product = keep_ref[n * NEAR]
            for m in range(1, NEAR):
                product = product * keep_ref[n * NEAR + m]
            far.append(lane_product(product))
        return near, far

    def weights(near, far):
        after = jnp.ones((batch, LANES), jnp.float32)
        for m in reversed(range(NEAR)):
            for s in range(batch):
                factor = spread(after[s : s + 1])
                for part in range(2):
                    total_ref[part, m, s] = factor * block_ref[part, 2 * NEAR - 1 - m]
            after = after * near[m]
        after = jnp.ones((batch, LANES), jnp.float32)
        for m in reversed(range(NEAR)):
            for s in range(batch):
                factor = spread(after[s : s + 1])
                for part in range(2):
                    inside_ref[part, m, s] = factor * block_ref[part, NEAR - 1 + at - m]
            after = after * jnp.where(m < at, near[m], 1.0)
        weight = (block_ref[0, NEAR + at], block_ref[1, NEAR + at])
        jump = (run_ref[0], run_ref[1])
        for d in range(1, FAR):
            for s in range(batch):
                factor = spread(after[s : s + 1])
                for part in range(2):
                    lines_ref[part, d - 1, s] = factor * weight[part]
            if d < FAR - 1:
                before = far[0]
                for m in range(1, FAR):
                    before = jnp.where(run - d == m, far[m], before)
                after = after * before
                weight = times(weight, jump)

    loads[2].wait()
    pieces[0].wait()
    found = scan(0)
    loads[3].wait()
    for s in range(1, batch):
        pieces[s].wait()
        if s == 1:
            products = block_products()
        if s == batch - 1:
            weights(*products)
        chain(s - 1, *found)
        found = scan(s)
    chain(batch - 1, *found)


def gathered(terms, flip):
    direct = cross = None
    for real, imag, x in terms:
        one, two = real * x, imag * x
        direct, cross = (one, two) if direct is None else (direct + one, cross + two)
    return direct + flip * swapped(cross)


def second(batch, got_ref, total_ref, send_ref):
    flip = sign()
    for s in range(batch):
        send_ref[s] = gathered([(total_ref[0, m, s], total_ref[1, m, s], got_ref[m, s]) for m in range(NEAR)], flip)


def third(batch, length, local_ref, near_ref, start_ref, chunk_ref, step_ref, reach_ref, decay_ref, inside_ref, lines_ref,
          *rest):
    far_refs, (y_hbm, y_ref, sems) = rest[: len(SENDS)], rest[len(SENDS) :]
    run = lax.axis_index("seq") // NEAR
    chunks = length // STEP
    part = chunks // 2
    size = part * STEP * ROWS
    flip = sign()
    stores = []
    for s in range(batch):
        terms = [(inside_ref[0, m, s], inside_ref[1, m, s], near_ref[m, s]) for m in range(NEAR)]
        for sends, far_ref in zip(SENDS, reversed(far_refs)):
            d = sum(jnp.where(run == to, to - at - 1, 0) for at, to, _ in sends)
            terms.append((lines_ref[0, d, s], lines_ref[1, d, s], far_ref[s]))
        carry = gathered(terms, flip)
        spun = flip * swapped(carry)
        for half in range(2):
            for k in range(half * part, half * part + part):
                entry = start_ref[s, k] + spread(reach_ref[pl.ds(s * chunks + k, 1)]) * (
                    chunk_ref[0, k] * carry + chunk_ref[1, k] * spun
                )
                turned = flip * swapped(entry)
                for i in range(STEP):
                    t = k * STEP + i
                    decay = spread(decay_ref[pl.ds(s * length + t, 1)])
                    state = local_ref[s, t] + decay * (step_ref[0, i] * entry + step_ref[1, i] * turned)
                    y_ref[pl.ds((s * length + t) * ROWS, ROWS)] = state.astype(jnp.bfloat16)
            rows = pl.ds((2 * s + half) * size, size)
            store = pltpu.make_async_copy(y_ref.at[rows], y_hbm.at[rows], sems.at[2 * s + half])
            store.start()
            stores.append(store)
    for store in stores:
        store.wait()


def shards(inputs, decay_rate, phase, keep):
    batch, length, parts, width = inputs.shape
    tiles = width // LANES
    blocks = keep.shape[1] // length
    chunks = length // STEP
    f32 = functools.partial(jax.ShapeDtypeStruct, dtype=jnp.float32)
    tile = (ROWS, LANES)
    total = batch * length * ROWS
    x = inputs.reshape(batch, length, parts, tiles, LANES).transpose(0, 1, 3, 2, 4).reshape(total, LANES)
    kept = keep.reshape(batch, blocks, length).transpose(1, 0, 2)
    given = (x, decay_rate.reshape(tiles, LANES), phase.reshape(tiles, LANES), kept)
    local, send, start, chunk, step, reach, decay, totals, inside, lines = pl.pallas_call(
        functools.partial(first, batch, length),
        out_shape=[
            f32((batch, length, *tile)),
            f32((NEAR, batch, *tile)),
            f32((batch, chunks, *tile)),
            f32((2, chunks, *tile)),
            f32((2, STEP, *tile)),
            f32((batch * chunks, LANES)),
            f32((batch * length, LANES)),
            f32((2, NEAR, batch, *tile)),
            f32((2, NEAR, batch, *tile)),
            f32((2, FAR - 1, batch, *tile)),
        ],
        in_specs=[HBM] * 4,
        out_specs=[VMEM] * 10,
        scratch_shapes=[
            pltpu.VMEM((total, LANES), jnp.bfloat16),
            pltpu.VMEM((blocks, batch, LANES), jnp.float32),
            pltpu.VMEM((2, tiles, LANES), jnp.float32),
            pltpu.SMEM((batch, LANES), jnp.float32),
            pltpu.VMEM((2, 2 * NEAR, *tile), jnp.float32),
            pltpu.VMEM((2, *tile), jnp.float32),
            pltpu.SemaphoreType.DMA((4 + batch,)),
        ],
        compiler_params=LIMIT,
    )(*(pltpu.with_memory_space_constraint(value, pltpu.HBM) for value in given))

    runs = range(blocks // NEAR)
    near = lax.all_to_all(
        send.reshape(NEAR, batch * ROWS, LANES),
        "seq",
        0,
        0,
        axis_index_groups=[[run * NEAR + m for m in range(NEAR)] for run in runs],
        tiled=True,
    ).reshape(send.shape)
    sums = pl.pallas_call(
        functools.partial(second, batch),
        out_shape=f32((batch, *tile)),
        in_specs=[VMEM] * 2,
        out_specs=VMEM,
        compiler_params=LIMIT,
    )(near, totals)
    flat = sums.reshape(batch * ROWS, LANES)
    far = []
    for sends in SENDS:
        pairs = [
            (at * NEAR + m, to * NEAR + (m + cross * WIDE) % NEAR) for at, to, cross in sends for m in range(NEAR)
        ]
        far.append(lax.ppermute(flat, "seq", pairs).reshape(sums.shape))
    y = pl.pallas_call(
        functools.partial(third, batch, length),
        out_shape=jax.ShapeDtypeStruct((total, LANES), jnp.bfloat16),
        in_specs=[VMEM] * (9 + len(SENDS)),
        out_specs=HBM,
        scratch_shapes=[
            pltpu.VMEM((total, LANES), jnp.bfloat16),
            pltpu.SemaphoreType.DMA((2 * batch,)),
        ],
        compiler_params=LIMIT,
    )(local, near, start, chunk, step, reach, decay, inside, lines, *reversed(far))
    y = y.reshape(batch, length, tiles, parts, LANES).transpose(0, 1, 3, 2, 4)
    return y.reshape(inputs.shape)


def solution(mesh):
    split = Mesh(mesh.devices, ("chan", "seq"))
    return jax.shard_map(
        shards,
        mesh=split,
        in_specs=(P(None, "seq", None, "chan"), P("chan"), P("chan"), P()),
        out_specs=P(None, "seq", None, "chan"),
        check_vma=False,
    )
```

```python
import functools

import jax
import jax.numpy as jnp
from jax import lax
from jax.experimental import pallas as pl
from jax.experimental.pallas import tpu as pltpu
from jax.sharding import Mesh
from jax.sharding import PartitionSpec as P

LANES = 128
ROWS = 8
STEP = 16
NEAR = 16
FAR = 4
WIDE = 8
SENDS = (
    ((0, 1, 0),),
    ((0, 3, 0),),
    ((0, 2, 1), (1, 3, 1)),
    ((1, 2, 0), (2, 3, 0)),
)

HBM = pl.BlockSpec(memory_space=pltpu.HBM)
VMEM = pl.BlockSpec(memory_space=pltpu.VMEM)
LIMIT = pltpu.CompilerParams(vmem_limit_bytes=8 * 1024 * 1024)


def times(one, two):
    a, b = one
    c, d = two
    return (a * c - b * d, a * d + b * c)


def powers(base, count):
    found = [None, base]
    for n in range(2, count):
        found.append(times(found[n // 2], found[n - n // 2]))
    return found


def places():
    return lax.broadcasted_iota(jnp.int32, (ROWS, LANES), 0)


def sign():
    return jnp.where(places() % 2 == 0, -1.0, 1.0)


def swapped(value):
    return jnp.take_along_axis(value, places() ^ 1, axis=0, mode="promise_in_bounds")


def spread(row):
    return jnp.broadcast_to(row, (ROWS, LANES))


def doubled(rows):
    return jnp.concatenate([rows[j // 2 : j // 2 + 1] for j in range(ROWS)], axis=0)


TURNS = ((1, 4), (4, 4), (16, 4), (64, 2))


def turned_product(value, width, turns):
    rolled = [value] + [pltpu.roll(value, width * n, 1) for n in range(1, turns)]
    while len(rolled) > 1:
        rolled = [rolled[n] * rolled[n + 1] for n in range(0, len(rolled), 2)]
    return rolled[0]


def lane_product(value):
    for width, turns in TURNS:
        value = turned_product(value, width, turns)
    return value


def windows(value):
    for width, turns in TURNS[:2]:
        value = turned_product(value, width, turns)
    return value


def minus_expm1_twice(rate):
    u = 2.0 * rate
    series = u * (1.0 - u / 2 * (1.0 - u / 3 * (1.0 - u / 4 * (1.0 - u / 5 * (1.0 - u / 6)))))
    return jnp.where(u < 0.1, series, 1.0 - jnp.exp(-u))


def first(batch, length, x_hbm, rate_hbm, phase_hbm, keep_hbm, x_ref, send_ref, ends_ref, step_ref, chunk_ref, block_ref,
          small_ref, ended_ref, kept_ref, total_ref, near_ref, keep_ref, param_ref, own_ref, sems):
    me = lax.axis_index("seq")
    run = me // NEAR
    chunks = length // STEP
    span = length * ROWS
    pieces = [
        pltpu.make_async_copy(x_hbm.at[pl.ds(s * span, span)], x_ref.at[pl.ds(s * span, span)], sems.at[4 + s])
        for s in range(batch)
    ]
    loads = [
        pltpu.make_async_copy(rate_hbm, param_ref.at[0], sems.at[0]),
        pltpu.make_async_copy(phase_hbm, param_ref.at[1], sems.at[1]),
        pltpu.make_async_copy(keep_hbm.at[me], own_ref.at[pl.ds(0, batch)], sems.at[2]),
        pltpu.make_async_copy(keep_hbm, keep_ref, sems.at[3]),
    ]
    own_ref[...] = jnp.ones_like(own_ref)
    for load in loads[:3] + pieces[:1] + loads[3:] + pieces[1:]:
        load.start()
    flip = sign()
    loads[0].wait()
    loads[1].wait()
    loads[2].wait()
    own = own_ref[...]
    upright = jnp.transpose(own)
    for s in range(batch):
        for t in range(0, length, ROWS):
            kept_ref[s, pl.ds(t, ROWS)] = jnp.broadcast_to(upright[t : t + ROWS, s : s + 1], (ROWS, LANES))
    ended = windows(own)
    rate, phase = doubled(param_ref[0]), doubled(param_ref[1])
    magnitude = jnp.exp(-rate)
    one, zero = jnp.ones_like(rate), jnp.zeros_like(rate)
    lam = (magnitude * jnp.cos(phase), magnitude * jnp.sin(phase))
    gamma = jnp.sqrt(minus_expm1_twice(rate))
    step = powers(lam, STEP + 1)
    chunk = powers(step[STEP], chunks + 1)
    block = powers(chunk[chunks], NEAR + 1)
    small_ref[0] = gamma
    for part in range(2):
        small_ref[1 + part] = block[NEAR][part]
        for n in range(STEP):
            step_ref[part, n] = step[n + 1][part]
        chunk_ref[part, 0] = zero if part else one
        for n in range(1, chunks):
            chunk_ref[part, n] = chunk[n][part]
        for n in range(NEAR):
            block_ref[part, n] = zero
        block_ref[part, NEAR] = zero if part else one
        for n in range(1, NEAR):
            block_ref[part, NEAR + n] = block[n][part]

    def ends(s):
        direct, cross = [None] * chunks, [None] * chunks
        for i in range(STEP):
            n = STEP - 1 - i
            for k in range(chunks):
                t = k * STEP + i
                x = x_ref[pl.ds(s * span + t * ROWS, ROWS)].astype(jnp.float32)
                if i == 0:
                    direct[k], cross[k] = step[n][0] * x, step[n][1] * x
                    continue
                kept = spread(kept_ref[s, pl.ds(t, 1)])
                direct[k] = kept * direct[k] + (step[n][0] * x if n else x)
                cross[k] = kept * cross[k] + step[n][1] * x if n else kept * cross[k]
        one_way = other = None
        for k in range(chunks):
            ends_ref[s, k, 0], ends_ref[s, k, 1] = direct[k], cross[k]
            last = k * STEP + STEP - 1
            decay = jnp.broadcast_to(ended[s : s + 1, last : last + 1], (ROWS, LANES))
            ended_ref[pl.ds(s * chunks + k, 1)] = decay[:1]
            if k < chunks - 1:
                n = chunks - 1 - k
                real = chunk[n][0] * direct[k] - chunk[n][1] * cross[k]
                imag = chunk[n][0] * cross[k] + chunk[n][1] * direct[k]
            else:
                real, imag = direct[k], cross[k]
            one_way, other = (real, imag) if k == 0 else (decay * one_way + real, decay * other + imag)
        state = gamma * (one_way + flip * swapped(other))
        for n in range(NEAR):
            send_ref[n, s] = state

    def weights(near):
        after = jnp.ones((batch, LANES), jnp.float32)
        for m in reversed(range(NEAR)):
            near_ref[m] = near[m]
            for s in range(batch):
                factor = spread(after[s : s + 1])
                for part in range(2):
                    total_ref[part, m, s] = factor * block_ref[part, 2 * NEAR - 1 - m]
            after = after * near[m]

    pieces[0].wait()
    ends(0)
    loads[3].wait()
    pieces[1].wait()
    near = [keep_ref[run * NEAR + m] for m in range(NEAR)]
    for width, turns in TURNS[:2]:
        near = [turned_product(value, width, turns) for value in near]
    ends(1)
    pieces[2].wait()
    for width, turns in TURNS[2:]:
        near = [turned_product(value, width, turns) for value in near]
    weights(near)
    ends(2)


def gathered(terms, flip):
    direct = cross = None
    for real, imag, x in terms:
        one, two = real * x, imag * x
        direct, cross = (one, two) if direct is None else (direct + one, cross + two)
    return direct + flip * swapped(cross)


def second(batch, got_ref, total_ref, send_ref):
    flip = sign()
    for s in range(batch):
        send_ref[s] = gathered([(total_ref[0, m, s], total_ref[1, m, s], got_ref[m, s]) for m in range(NEAR)], flip)


def middle(batch, length, x_ref, got_ref, ends_ref, step_ref, chunk_ref, block_ref, small_ref, ended_ref, kept_ref,
           near_ref, keep_ref, local_ref, decay_ref, inside_ref, lines_ref):
    me = lax.axis_index("seq")
    run, at = me // NEAR, me % NEAR
    chunks = length // STEP
    span = length * ROWS
    flip = sign()
    products = []
    for n in range(FAR):
        product = keep_ref[n * NEAR]
        for m in range(1, NEAR):
            product = product * keep_ref[n * NEAR + m]
        products.append(product)
    back = []
    for d in range(1, FAR - 1):
        before = products[0]
        for m in range(1, FAR):
            before = jnp.where(run - d == m, products[m], before)
        back.append(lane_product(before))

    gamma = small_ref[0]
    lam_re, lam_im = step_ref[0, 0], step_ref[1, 0] * flip
    jump_re, jump_im = step_ref[0, STEP - 1], step_ref[1, STEP - 1] * flip
    state, reach = {}, {}
    for s in range(batch):
        for k in range(chunks):
            if k == 0:
                state[s, k], reach[s, k] = jnp.zeros_like(gamma), jnp.ones_like(gamma)
                continue
            h = state[s, k - 1]
            decay = spread(ended_ref[pl.ds(s * chunks + k - 1, 1)])
            end = gamma * (ends_ref[s, k - 1, 0] + flip * swapped(ends_ref[s, k - 1, 1]))
            state[s, k] = decay * (jump_re * h + jump_im * swapped(h)) + end
            reach[s, k] = decay * reach[s, k - 1]
    for k in range(chunks):
        for i in range(STEP):
            t = k * STEP + i
            power = times((step_ref[0, i], step_ref[1, i]), (chunk_ref[0, k], chunk_ref[1, k]))
            for s in range(batch):
                kept = spread(kept_ref[s, pl.ds(t, 1)])
                x = gamma * x_ref[pl.ds(s * span + t * ROWS, ROWS)].astype(jnp.float32)
                h = state[s, k]
                state[s, k] = kept * (lam_re * h + lam_im * swapped(h)) + x
                reach[s, k] = kept * reach[s, k]
                local_ref[s, t] = state[s, k]
                for part in range(2):
                    decay_ref[part, s, t] = reach[s, k] * power[part]

    after = jnp.ones((batch, LANES), jnp.float32)
    terms = [[] for _ in range(batch)]
    for m in reversed(range(NEAR)):
        real, imag = block_ref[0, NEAR - 1 + at - m], block_ref[1, NEAR - 1 + at - m]
        for s in range(batch):
            factor = spread(after[s : s + 1])
            terms[s].append((factor * real, factor * imag, got_ref[m, s]))
        after = after * jnp.where(m < at, near_ref[m], 1.0)
    for s in range(batch):
        inside_ref[s] = gathered(terms[s], flip)
    weight = (block_ref[0, NEAR + at], block_ref[1, NEAR + at])
    for d in range(1, FAR):
        for s in range(batch):
            factor = spread(after[s : s + 1])
            for part in range(2):
                lines_ref[part, d - 1, s] = factor * weight[part]
        if d < FAR - 1:
            after = after * back[d - 1]
            weight = times(weight, (small_ref[1], small_ref[2]))


def third(batch, length, local_ref, decay_ref, inside_ref, lines_ref, *rest):
    far_refs, (y_hbm, y_ref, sems) = rest[: len(SENDS)], rest[len(SENDS) :]
    run = lax.axis_index("seq") // NEAR
    flip = sign()
    size = length // 2
    stores = []
    for s in range(batch):
        terms = []
        for sends, far_ref in zip(SENDS, reversed(far_refs)):
            d = sum(jnp.where(run == to, to - at - 1, 0) for at, to, _ in sends)
            terms.append((lines_ref[0, d, s], lines_ref[1, d, s], far_ref[s]))
        carry = inside_ref[s] + gathered(terms, flip)
        turned = flip * swapped(carry)
        for half in range(2):
            for t in range(half * size, half * size + size):
                state = local_ref[s, t] + (decay_ref[0, s, t] * carry + decay_ref[1, s, t] * turned)
                y_ref[pl.ds((s * length + t) * ROWS, ROWS)] = state.astype(jnp.bfloat16)
            rows = pl.ds((2 * s + half) * size * ROWS, size * ROWS)
            store = pltpu.make_async_copy(y_ref.at[rows], y_hbm.at[rows], sems.at[2 * s + half])
            store.start()
            stores.append(store)
    for store in stores:
        store.wait()


def shards(inputs, decay_rate, phase, keep):
    batch, length, parts, width = inputs.shape
    tiles = width // LANES
    blocks = keep.shape[1] // length
    chunks = length // STEP
    f32 = functools.partial(jax.ShapeDtypeStruct, dtype=jnp.float32)
    tile = (ROWS, LANES)
    total = batch * length * ROWS
    x = inputs.reshape(batch, length, parts, tiles, LANES).transpose(0, 1, 3, 2, 4).reshape(total, LANES)
    kept = keep.reshape(batch, blocks, length).transpose(1, 0, 2)
    given = (x, decay_rate.reshape(tiles, LANES), phase.reshape(tiles, LANES), kept)
    x, send, ends, step, chunk, block, small, ended, kepts, totals, products, keeps = pl.pallas_call(
        functools.partial(first, batch, length),
        out_shape=[
            jax.ShapeDtypeStruct((total, LANES), jnp.bfloat16),
            f32((NEAR, batch, *tile)),
            f32((batch, chunks, 2, *tile)),
            f32((2, STEP, *tile)),
            f32((2, chunks, *tile)),
            f32((2, 2 * NEAR, *tile)),
            f32((3, *tile)),
            f32((batch * chunks, LANES)),
            f32((batch, length, LANES)),
            f32((2, NEAR, batch, *tile)),
            f32((NEAR, batch, LANES)),
            f32((blocks, batch, LANES)),
        ],
        in_specs=[HBM] * 4,
        out_specs=[VMEM] * 12,
        scratch_shapes=[
            pltpu.VMEM((2, tiles, LANES), jnp.float32),
            pltpu.VMEM((ROWS, LANES), jnp.float32),
            pltpu.SemaphoreType.DMA((4 + batch,)),
        ],
        compiler_params=LIMIT,
    )(*(pltpu.with_memory_space_constraint(value, pltpu.HBM) for value in given))

    runs = range(blocks // NEAR)
    near = lax.all_to_all(
        send.reshape(NEAR, batch * ROWS, LANES),
        "seq",
        0,
        0,
        axis_index_groups=[[run * NEAR + m for m in range(NEAR)] for run in runs],
        tiled=True,
    ).reshape(send.shape)
    sums = pl.pallas_call(
        functools.partial(second, batch),
        out_shape=f32((batch, *tile)),
        in_specs=[VMEM] * 2,
        out_specs=VMEM,
        compiler_params=LIMIT,
    )(near, totals)
    flat = sums.reshape(batch * ROWS, LANES)
    far = []
    for sends in SENDS:
        pairs = [
            (at * NEAR + m, to * NEAR + (m + cross * WIDE) % NEAR) for at, to, cross in sends for m in range(NEAR)
        ]
        far.append(lax.ppermute(flat, "seq", pairs).reshape(sums.shape))
    local, decay, inside, lines = pl.pallas_call(
        functools.partial(middle, batch, length),
        out_shape=[
            f32((batch, length, *tile)),
            f32((2, batch, length, *tile)),
            f32((batch, *tile)),
            f32((2, FAR - 1, batch, *tile)),
        ],
        in_specs=[VMEM] * 11,
        out_specs=[VMEM] * 4,
        compiler_params=LIMIT,
        cost_estimate=pl.CostEstimate(flops=10_000_000, bytes_accessed=6_000_000, transcendentals=0),
    )(x, near, ends, step, chunk, block, small, ended, kepts, products, keeps)
    y = pl.pallas_call(
        functools.partial(third, batch, length),
        out_shape=jax.ShapeDtypeStruct((total, LANES), jnp.bfloat16),
        in_specs=[VMEM] * (4 + len(SENDS)),
        out_specs=HBM,
        scratch_shapes=[
            pltpu.VMEM((total, LANES), jnp.bfloat16),
            pltpu.SemaphoreType.DMA((2 * batch,)),
        ],
        compiler_params=LIMIT,
    )(local, decay, inside, lines, *reversed(far))
    y = y.reshape(batch, length, tiles, parts, LANES).transpose(0, 1, 3, 2, 4)
    return y.reshape(inputs.shape)


def solution(mesh):
    split = Mesh(mesh.devices, ("chan", "seq"))
    return jax.shard_map(
        shards,
        mesh=split,
        in_specs=(P(None, "seq", None, "chan"), P("chan"), P("chan"), P()),
        out_specs=P(None, "seq", None, "chan"),
        check_vma=False,
    )
```

```python
import functools

import jax
import jax.numpy as jnp
from jax import lax
from jax.experimental import pallas as pl
from jax.experimental.pallas import tpu as pltpu
from jax.sharding import Mesh
from jax.sharding import PartitionSpec as P

LANES = 128
ROWS = 8
STEP = 16
NEAR = 16
FAR = 4
WIDE = 8
SENDS = (
    ((0, 1, 0),),
    ((0, 3, 0),),
    ((0, 2, 1), (1, 3, 1)),
    ((1, 2, 0), (2, 3, 0)),
)

HBM = pl.BlockSpec(memory_space=pltpu.HBM)
VMEM = pl.BlockSpec(memory_space=pltpu.VMEM)
LIMIT = pltpu.CompilerParams(vmem_limit_bytes=8 * 1024 * 1024)


def times(one, two):
    a, b = one
    c, d = two
    return (a * c - b * d, a * d + b * c)


def powers(base, count):
    found = [None, base]
    for n in range(2, count):
        found.append(times(found[n // 2], found[n - n // 2]))
    return found


def places():
    return lax.broadcasted_iota(jnp.int32, (ROWS, LANES), 0)


def sign():
    return jnp.where(places() % 2 == 0, -1.0, 1.0)


def swapped(value):
    return jnp.take_along_axis(value, places() ^ 1, axis=0, mode="promise_in_bounds")


def spread(row):
    return jnp.broadcast_to(row, (ROWS, LANES))


def doubled(rows):
    return jnp.concatenate([rows[j // 2 : j // 2 + 1] for j in range(ROWS)], axis=0)


TURNS = ((1, 4), (4, 4), (16, 4), (64, 2))


def turned_product(value, width, turns):
    rolled = [value] + [pltpu.roll(value, width * n, 1) for n in range(1, turns)]
    while len(rolled) > 1:
        rolled = [rolled[n] * rolled[n + 1] for n in range(0, len(rolled), 2)]
    return rolled[0]


def lane_product(value):
    for width, turns in TURNS:
        value = turned_product(value, width, turns)
    return value


def windows(value):
    for width, turns in TURNS[:2]:
        value = turned_product(value, width, turns)
    return value


def minus_expm1_twice(rate):
    u = 2.0 * rate
    series = u * (1.0 - u / 2 * (1.0 - u / 3 * (1.0 - u / 4 * (1.0 - u / 5 * (1.0 - u / 6)))))
    return jnp.where(u < 0.1, series, 1.0 - jnp.exp(-u))


def first(batch, length, x_hbm, rate_hbm, phase_hbm, keep_hbm, x_ref, send_ref, ends_ref, step_ref, chunk_ref, block_ref,
          small_ref, ended_ref, kept_ref, total_ref, near_ref, keep_ref, param_ref, own_ref, sems):
    me = lax.axis_index("seq")
    run = me // NEAR
    chunks = length // STEP
    span = length * ROWS
    pieces = [
        pltpu.make_async_copy(x_hbm.at[pl.ds(s * span, span)], x_ref.at[pl.ds(s * span, span)], sems.at[4 + s])
        for s in range(batch)
    ]
    loads = [
        pltpu.make_async_copy(rate_hbm, param_ref.at[0], sems.at[0]),
        pltpu.make_async_copy(phase_hbm, param_ref.at[1], sems.at[1]),
        pltpu.make_async_copy(keep_hbm.at[me], own_ref.at[pl.ds(0, batch)], sems.at[2]),
        pltpu.make_async_copy(keep_hbm, keep_ref, sems.at[3]),
    ]
    own_ref[...] = jnp.ones_like(own_ref)
    for load in loads[:3] + pieces[:1] + loads[3:] + pieces[1:]:
        load.start()
    flip = sign()
    loads[0].wait()
    loads[1].wait()
    loads[2].wait()
    own = own_ref[...]
    upright = jnp.transpose(own)
    for s in range(batch):
        for t in range(0, length, ROWS):
            kept_ref[s, pl.ds(t, ROWS)] = jnp.broadcast_to(upright[t : t + ROWS, s : s + 1], (ROWS, LANES))
    ended = windows(own)
    rate, phase = doubled(param_ref[0]), doubled(param_ref[1])
    magnitude = jnp.exp(-rate)
    one, zero = jnp.ones_like(rate), jnp.zeros_like(rate)
    lam = (magnitude * jnp.cos(phase), magnitude * jnp.sin(phase))
    gamma = jnp.sqrt(minus_expm1_twice(rate))
    step = powers(lam, STEP + 1)
    chunk = powers(step[STEP], chunks + 1)
    block = powers(chunk[chunks], NEAR + 1)
    small_ref[0] = gamma
    for part in range(2):
        small_ref[1 + part] = block[NEAR][part]
        for n in range(STEP):
            step_ref[part, n] = step[n + 1][part]
        chunk_ref[part, 0] = zero if part else one
        for n in range(1, chunks):
            chunk_ref[part, n] = chunk[n][part]
        for n in range(NEAR):
            block_ref[part, n] = zero
        block_ref[part, NEAR] = zero if part else one
        for n in range(1, NEAR):
            block_ref[part, NEAR + n] = block[n][part]

    def ends(s):
        direct, cross = [None] * chunks, [None] * chunks
        for i in range(STEP):
            n = STEP - 1 - i
            for k in range(chunks):
                t = k * STEP + i
                x = x_ref[pl.ds(s * span + t * ROWS, ROWS)].astype(jnp.float32)
                if i == 0:
                    direct[k], cross[k] = step[n][0] * x, step[n][1] * x
                    continue
                kept = spread(kept_ref[s, pl.ds(t, 1)])
                direct[k] = kept * direct[k] + (step[n][0] * x if n else x)
                cross[k] = kept * cross[k] + step[n][1] * x if n else kept * cross[k]
        one_way = other = None
        for k in range(chunks):
            ends_ref[s, k, 0], ends_ref[s, k, 1] = direct[k], cross[k]
            last = k * STEP + STEP - 1
            decay = jnp.broadcast_to(ended[s : s + 1, last : last + 1], (ROWS, LANES))
            ended_ref[pl.ds(s * chunks + k, 1)] = decay[:1]
            if k < chunks - 1:
                n = chunks - 1 - k
                real = chunk[n][0] * direct[k] - chunk[n][1] * cross[k]
                imag = chunk[n][0] * cross[k] + chunk[n][1] * direct[k]
            else:
                real, imag = direct[k], cross[k]
            one_way, other = (real, imag) if k == 0 else (decay * one_way + real, decay * other + imag)
        state = gamma * (one_way + flip * swapped(other))
        for n in range(NEAR):
            send_ref[n, s] = state

    def weights(near):
        after = jnp.ones((batch, LANES), jnp.float32)
        for m in reversed(range(NEAR)):
            near_ref[m] = near[m]
            for s in range(batch):
                factor = spread(after[s : s + 1])
                for part in range(2):
                    total_ref[part, m, s] = factor * block_ref[part, 2 * NEAR - 1 - m]
            after = after * near[m]

    pieces[0].wait()
    ends(0)
    loads[3].wait()
    pieces[1].wait()
    near = [keep_ref[run * NEAR + m] for m in range(NEAR)]
    for width, turns in TURNS[:2]:
        near = [turned_product(value, width, turns) for value in near]
    ends(1)
    pieces[2].wait()
    for width, turns in TURNS[2:]:
        near = [turned_product(value, width, turns) for value in near]
    weights(near)
    ends(2)


def gathered(terms, flip):
    direct = cross = None
    for real, imag, x in terms:
        one, two = real * x, imag * x
        direct, cross = (one, two) if direct is None else (direct + one, cross + two)
    return direct + flip * swapped(cross)


def second(batch, got_ref, total_ref, send_ref):
    flip = sign()
    for s in range(batch):
        send_ref[s] = gathered([(total_ref[0, m, s], total_ref[1, m, s], got_ref[m, s]) for m in range(NEAR)], flip)


def middle(batch, length, x_ref, got_ref, ends_ref, step_ref, chunk_ref, block_ref, small_ref, ended_ref, kept_ref,
           near_ref, keep_ref, local_ref, decay_ref, inside_ref, lines_ref):
    me = lax.axis_index("seq")
    run, at = me // NEAR, me % NEAR
    chunks = length // STEP
    span = length * ROWS
    flip = sign()
    products = []
    for n in range(FAR):
        product = keep_ref[n * NEAR]
        for m in range(1, NEAR):
            product = product * keep_ref[n * NEAR + m]
        products.append(product)
    back = []
    for d in range(1, FAR - 1):
        before = products[0]
        for m in range(1, FAR):
            before = jnp.where(run - d == m, products[m], before)
        back.append(lane_product(before))

    gamma = small_ref[0]
    lam_re, lam_im = step_ref[0, 0], step_ref[1, 0] * flip
    jump_re, jump_im = step_ref[0, STEP - 1], step_ref[1, STEP - 1] * flip
    state, reach = {}, {}
    for s in range(batch):
        for k in range(chunks):
            if k == 0:
                state[s, k], reach[s, k] = jnp.zeros_like(gamma), jnp.ones_like(gamma)
                continue
            h = state[s, k - 1]
            decay = spread(ended_ref[pl.ds(s * chunks + k - 1, 1)])
            end = gamma * (ends_ref[s, k - 1, 0] + flip * swapped(ends_ref[s, k - 1, 1]))
            state[s, k] = decay * (jump_re * h + jump_im * swapped(h)) + end
            reach[s, k] = decay * reach[s, k - 1]
    for k in range(chunks):
        for i in range(STEP):
            t = k * STEP + i
            power = times((step_ref[0, i], step_ref[1, i]), (chunk_ref[0, k], chunk_ref[1, k]))
            for s in range(batch):
                kept = spread(kept_ref[s, pl.ds(t, 1)])
                x = gamma * x_ref[pl.ds(s * span + t * ROWS, ROWS)].astype(jnp.float32)
                h = state[s, k]
                state[s, k] = kept * (lam_re * h + lam_im * swapped(h)) + x
                reach[s, k] = kept * reach[s, k]
                local_ref[s, t] = state[s, k]
                for part in range(2):
                    decay_ref[part, s, t] = reach[s, k] * power[part]

    after = jnp.ones((batch, LANES), jnp.float32)
    terms = [[] for _ in range(batch)]
    for m in reversed(range(NEAR)):
        real, imag = block_ref[0, NEAR - 1 + at - m], block_ref[1, NEAR - 1 + at - m]
        for s in range(batch):
            factor = spread(after[s : s + 1])
            terms[s].append((factor * real, factor * imag, got_ref[m, s]))
        after = after * jnp.where(m < at, near_ref[m], 1.0)
    for s in range(batch):
        inside_ref[s] = gathered(terms[s], flip)
    weight = (block_ref[0, NEAR + at], block_ref[1, NEAR + at])
    for d in range(1, FAR):
        for s in range(batch):
            factor = spread(after[s : s + 1])
            for part in range(2):
                lines_ref[part, d - 1, s] = factor * weight[part]
        if d < FAR - 1:
            after = after * back[d - 1]
            weight = times(weight, (small_ref[1], small_ref[2]))


def third(batch, length, local_ref, decay_ref, inside_ref, lines_ref, *rest):
    far_refs, (y_hbm, y_ref, sems) = rest[: len(SENDS)], rest[len(SENDS) :]
    run = lax.axis_index("seq") // NEAR
    flip = sign()
    size = length // 2
    stores = []
    for s in range(batch):
        terms = []
        for sends, far_ref in zip(SENDS, reversed(far_refs)):
            d = sum(jnp.where(run == to, to - at - 1, 0) for at, to, _ in sends)
            terms.append((lines_ref[0, d, s], lines_ref[1, d, s], far_ref[s]))
        carry = inside_ref[s] + gathered(terms, flip)
        turned = flip * swapped(carry)
        for half in range(2):
            for t in range(half * size, half * size + size):
                state = local_ref[s, t] + (decay_ref[0, s, t] * carry + decay_ref[1, s, t] * turned)
                y_ref[pl.ds((s * length + t) * ROWS, ROWS)] = state.astype(jnp.bfloat16)
            rows = pl.ds((2 * s + half) * size * ROWS, size * ROWS)
            store = pltpu.make_async_copy(y_ref.at[rows], y_hbm.at[rows], sems.at[2 * s + half])
            store.start()
            stores.append(store)
    for store in stores:
        store.wait()


def shards(inputs, decay_rate, phase, keep):
    batch, length, parts, width = inputs.shape
    tiles = width // LANES
    blocks = keep.shape[1] // length
    chunks = length // STEP
    f32 = functools.partial(jax.ShapeDtypeStruct, dtype=jnp.float32)
    tile = (ROWS, LANES)
    total = batch * length * ROWS
    x = inputs.reshape(batch, length, parts, tiles, LANES).transpose(0, 1, 3, 2, 4).reshape(total, LANES)
    kept = keep.reshape(batch, blocks, length).transpose(1, 0, 2)
    given = (x, decay_rate.reshape(tiles, LANES), phase.reshape(tiles, LANES), kept)
    x, send, ends, step, chunk, block, small, ended, kepts, totals, products, keeps = pl.pallas_call(
        functools.partial(first, batch, length),
        out_shape=[
            jax.ShapeDtypeStruct((total, LANES), jnp.bfloat16),
            f32((NEAR, batch, *tile)),
            f32((batch, chunks, 2, *tile)),
            f32((2, STEP, *tile)),
            f32((2, chunks, *tile)),
            f32((2, 2 * NEAR, *tile)),
            f32((3, *tile)),
            f32((batch * chunks, LANES)),
            f32((batch, length, LANES)),
            f32((2, NEAR, batch, *tile)),
            f32((NEAR, batch, LANES)),
            f32((blocks, batch, LANES)),
        ],
        in_specs=[HBM] * 4,
        out_specs=[VMEM] * 12,
        scratch_shapes=[
            pltpu.VMEM((2, tiles, LANES), jnp.float32),
            pltpu.VMEM((ROWS, LANES), jnp.float32),
            pltpu.SemaphoreType.DMA((4 + batch,)),
        ],
        compiler_params=LIMIT,
    )(*(pltpu.with_memory_space_constraint(value, pltpu.HBM) for value in given))

    runs = range(blocks // NEAR)
    near = lax.all_to_all(
        send.reshape(NEAR, batch * ROWS, LANES),
        "seq",
        0,
        0,
        axis_index_groups=[[run * NEAR + m for m in range(NEAR)] for run in runs],
        tiled=True,
    ).reshape(send.shape)
    sums = pl.pallas_call(
        functools.partial(second, batch),
        out_shape=f32((batch, *tile)),
        in_specs=[VMEM] * 2,
        out_specs=VMEM,
        compiler_params=LIMIT,
    )(near, totals)
    flat = sums.reshape(batch * ROWS, LANES)
    far = []
    for sends in SENDS:
        pairs = [
            (at * NEAR + m, to * NEAR + ((m + cross * WIDE) % NEAR ^ 1)) for at, to, cross in sends for m in range(NEAR)
        ]
        far.append(lax.ppermute(flat, "seq", pairs).reshape(sums.shape))
    local, decay, inside, lines = pl.pallas_call(
        functools.partial(middle, batch, length),
        out_shape=[
            f32((batch, length, *tile)),
            f32((2, batch, length, *tile)),
            f32((batch, *tile)),
            f32((2, FAR - 1, batch, *tile)),
        ],
        in_specs=[VMEM] * 11,
        out_specs=[VMEM] * 4,
        compiler_params=LIMIT,
        cost_estimate=pl.CostEstimate(flops=10_000_000, bytes_accessed=6_000_000, transcendentals=0),
    )(x, near, ends, step, chunk, block, small, ended, kepts, products, keeps)
    y = pl.pallas_call(
        functools.partial(third, batch, length),
        out_shape=jax.ShapeDtypeStruct((total, LANES), jnp.bfloat16),
        in_specs=[VMEM] * (4 + len(SENDS)),
        out_specs=HBM,
        scratch_shapes=[
            pltpu.VMEM((total, LANES), jnp.bfloat16),
            pltpu.SemaphoreType.DMA((2 * batch,)),
        ],
        compiler_params=LIMIT,
    )(local, decay, inside, lines, *reversed(far))
    y = y.reshape(batch, length, tiles, parts, LANES).transpose(0, 1, 3, 2, 4)
    return y.reshape(inputs.shape)


def solution(mesh):
    split = Mesh(mesh.devices, ("chan", "seq"))
    return jax.shard_map(
        shards,
        mesh=split,
        in_specs=(P(None, "seq", None, "chan"), P("chan"), P("chan"), P()),
        out_specs=P(None, "seq", None, "chan"),
        check_vma=False,
    )
```

```python
import functools

import jax
import jax.numpy as jnp
from jax import lax
from jax.experimental import pallas as pl
from jax.experimental.pallas import tpu as pltpu
from jax.sharding import Mesh
from jax.sharding import PartitionSpec as P

LANES = 128
ROWS = 8
STEP = 16
NEAR = 16
FAR = 4
WIDE = 8
SENDS = (
    ((0, 1, 0),),
    ((0, 3, 1),),
    ((0, 2, 1), (1, 3, 1)),
    ((1, 2, 0), (2, 3, 1)),
)

HBM = pl.BlockSpec(memory_space=pltpu.HBM)
VMEM = pl.BlockSpec(memory_space=pltpu.VMEM)
LIMIT = pltpu.CompilerParams(vmem_limit_bytes=8 * 1024 * 1024)


def times(one, two):
    a, b = one
    c, d = two
    return (a * c - b * d, a * d + b * c)


def powers(base, count):
    found = [None, base]
    for n in range(2, count):
        found.append(times(found[n // 2], found[n - n // 2]))
    return found


def places():
    return lax.broadcasted_iota(jnp.int32, (ROWS, LANES), 0)


def sign():
    return jnp.where(places() % 2 == 0, -1.0, 1.0)


def swapped(value):
    return jnp.take_along_axis(value, places() ^ 1, axis=0, mode="promise_in_bounds")


def spread(row):
    return jnp.broadcast_to(row, (ROWS, LANES))


def doubled(rows):
    return jnp.concatenate([rows[j // 2 : j // 2 + 1] for j in range(ROWS)], axis=0)


TURNS = ((1, 4), (4, 4), (16, 4), (64, 2))


def turned_product(value, width, turns):
    rolled = [value] + [pltpu.roll(value, width * n, 1) for n in range(1, turns)]
    while len(rolled) > 1:
        rolled = [rolled[n] * rolled[n + 1] for n in range(0, len(rolled), 2)]
    return rolled[0]


def lane_product(value):
    for width, turns in TURNS:
        value = turned_product(value, width, turns)
    return value


def windows(value):
    for width, turns in TURNS[:2]:
        value = turned_product(value, width, turns)
    return value


def minus_expm1_twice(rate):
    u = 2.0 * rate
    series = u * (1.0 - u / 2 * (1.0 - u / 3 * (1.0 - u / 4 * (1.0 - u / 5 * (1.0 - u / 6)))))
    return jnp.where(u < 0.1, series, 1.0 - jnp.exp(-u))


def first(batch, length, x_hbm, rate_hbm, phase_hbm, keep_hbm, x_ref, send_ref, ends_ref, step_ref, chunk_ref, block_ref,
          small_ref, ended_ref, kept_ref, total_ref, near_ref, keep_ref, param_ref, own_ref, sems):
    me = lax.axis_index("seq")
    run = me // NEAR
    chunks = length // STEP
    span = length * ROWS
    pieces = [
        pltpu.make_async_copy(x_hbm.at[pl.ds(s * span, span)], x_ref.at[pl.ds(s * span, span)], sems.at[4 + s])
        for s in range(batch)
    ]
    loads = [
        pltpu.make_async_copy(rate_hbm, param_ref.at[0], sems.at[0]),
        pltpu.make_async_copy(phase_hbm, param_ref.at[1], sems.at[1]),
        pltpu.make_async_copy(keep_hbm.at[me], own_ref.at[pl.ds(0, batch)], sems.at[2]),
        pltpu.make_async_copy(keep_hbm, keep_ref, sems.at[3]),
    ]
    own_ref[...] = jnp.ones_like(own_ref)
    for load in loads[:3] + pieces[:1] + loads[3:] + pieces[1:]:
        load.start()
    flip = sign()
    loads[0].wait()
    loads[1].wait()
    loads[2].wait()
    own = own_ref[...]
    upright = jnp.transpose(own)
    for s in range(batch):
        for t in range(0, length, ROWS):
            kept_ref[s, pl.ds(t, ROWS)] = jnp.broadcast_to(upright[t : t + ROWS, s : s + 1], (ROWS, LANES))
    ended = windows(own)
    rate, phase = doubled(param_ref[0]), doubled(param_ref[1])
    magnitude = jnp.exp(-rate)
    one, zero = jnp.ones_like(rate), jnp.zeros_like(rate)
    lam = (magnitude * jnp.cos(phase), magnitude * jnp.sin(phase))
    gamma = jnp.sqrt(minus_expm1_twice(rate))
    step = powers(lam, STEP + 1)
    chunk = powers(step[STEP], chunks + 1)
    block = powers(chunk[chunks], NEAR + 1)
    small_ref[0] = gamma
    for part in range(2):
        small_ref[1 + part] = block[NEAR][part]
        for n in range(STEP):
            step_ref[part, n] = step[n + 1][part]
        chunk_ref[part, 0] = zero if part else one
        for n in range(1, chunks):
            chunk_ref[part, n] = chunk[n][part]
        for n in range(NEAR):
            block_ref[part, n] = zero
        block_ref[part, NEAR] = zero if part else one
        for n in range(1, NEAR):
            block_ref[part, NEAR + n] = block[n][part]

    def ends(s):
        direct, cross = [None] * chunks, [None] * chunks
        for i in range(STEP):
            n = STEP - 1 - i
            for k in range(chunks):
                t = k * STEP + i
                x = x_ref[pl.ds(s * span + t * ROWS, ROWS)].astype(jnp.float32)
                if i == 0:
                    direct[k], cross[k] = step[n][0] * x, step[n][1] * x
                    continue
                kept = spread(kept_ref[s, pl.ds(t, 1)])
                direct[k] = kept * direct[k] + (step[n][0] * x if n else x)
                cross[k] = kept * cross[k] + step[n][1] * x if n else kept * cross[k]
        one_way = other = None
        for k in range(chunks):
            ends_ref[s, k, 0], ends_ref[s, k, 1] = direct[k], cross[k]
            last = k * STEP + STEP - 1
            decay = jnp.broadcast_to(ended[s : s + 1, last : last + 1], (ROWS, LANES))
            ended_ref[pl.ds(s * chunks + k, 1)] = decay[:1]
            if k < chunks - 1:
                n = chunks - 1 - k
                real = chunk[n][0] * direct[k] - chunk[n][1] * cross[k]
                imag = chunk[n][0] * cross[k] + chunk[n][1] * direct[k]
            else:
                real, imag = direct[k], cross[k]
            one_way, other = (real, imag) if k == 0 else (decay * one_way + real, decay * other + imag)
        state = gamma * (one_way + flip * swapped(other))
        for n in range(NEAR):
            send_ref[n, s] = state

    def weights(near):
        after = jnp.ones((batch, LANES), jnp.float32)
        for m in reversed(range(NEAR)):
            near_ref[m] = near[m]
            for s in range(batch):
                factor = spread(after[s : s + 1])
                for part in range(2):
                    total_ref[part, m, s] = factor * block_ref[part, 2 * NEAR - 1 - m]
            after = after * near[m]

    pieces[0].wait()
    ends(0)
    loads[3].wait()
    pieces[1].wait()
    near = [keep_ref[run * NEAR + m] for m in range(NEAR)]
    for width, turns in TURNS[:2]:
        near = [turned_product(value, width, turns) for value in near]
    ends(1)
    pieces[2].wait()
    for width, turns in TURNS[2:]:
        near = [turned_product(value, width, turns) for value in near]
    weights(near)
    ends(2)


def gathered(terms, flip):
    direct = cross = None
    for real, imag, x in terms:
        one, two = real * x, imag * x
        direct, cross = (one, two) if direct is None else (direct + one, cross + two)
    return direct + flip * swapped(cross)


def second(batch, got_ref, total_ref, send_ref):
    flip = sign()
    for s in range(batch):
        send_ref[s] = gathered([(total_ref[0, m, s], total_ref[1, m, s], got_ref[m, s]) for m in range(NEAR)], flip)


def middle(batch, length, x_ref, got_ref, ends_ref, step_ref, chunk_ref, block_ref, small_ref, ended_ref, kept_ref,
           near_ref, keep_ref, local_ref, decay_ref, inside_ref, lines_ref):
    me = lax.axis_index("seq")
    run, at = me // NEAR, me % NEAR
    chunks = length // STEP
    span = length * ROWS
    flip = sign()
    products = []
    for n in range(FAR):
        product = keep_ref[n * NEAR]
        for m in range(1, NEAR):
            product = product * keep_ref[n * NEAR + m]
        products.append(product)
    back = []
    for d in range(1, FAR - 1):
        before = products[0]
        for m in range(1, FAR):
            before = jnp.where(run - d == m, products[m], before)
        back.append(lane_product(before))

    gamma = small_ref[0]
    lam_re, lam_im = step_ref[0, 0], step_ref[1, 0] * flip
    jump_re, jump_im = step_ref[0, STEP - 1], step_ref[1, STEP - 1] * flip
    state, reach = {}, {}
    for s in range(batch):
        for k in range(chunks):
            if k == 0:
                state[s, k], reach[s, k] = jnp.zeros_like(gamma), jnp.ones_like(gamma)
                continue
            h = state[s, k - 1]
            decay = spread(ended_ref[pl.ds(s * chunks + k - 1, 1)])
            end = gamma * (ends_ref[s, k - 1, 0] + flip * swapped(ends_ref[s, k - 1, 1]))
            state[s, k] = decay * (jump_re * h + jump_im * swapped(h)) + end
            reach[s, k] = decay * reach[s, k - 1]
    for k in range(chunks):
        for i in range(STEP):
            t = k * STEP + i
            power = times((step_ref[0, i], step_ref[1, i]), (chunk_ref[0, k], chunk_ref[1, k]))
            for s in range(batch):
                kept = spread(kept_ref[s, pl.ds(t, 1)])
                x = gamma * x_ref[pl.ds(s * span + t * ROWS, ROWS)].astype(jnp.float32)
                h = state[s, k]
                state[s, k] = kept * (lam_re * h + lam_im * swapped(h)) + x
                reach[s, k] = kept * reach[s, k]
                local_ref[s, t] = state[s, k]
                for part in range(2):
                    decay_ref[part, s, t] = reach[s, k] * power[part]

    after = jnp.ones((batch, LANES), jnp.float32)
    terms = [[] for _ in range(batch)]
    for m in reversed(range(NEAR)):
        real, imag = block_ref[0, NEAR - 1 + at - m], block_ref[1, NEAR - 1 + at - m]
        for s in range(batch):
            factor = spread(after[s : s + 1])
            terms[s].append((factor * real, factor * imag, got_ref[m, s]))
        after = after * jnp.where(m < at, near_ref[m], 1.0)
    for s in range(batch):
        inside_ref[s] = gathered(terms[s], flip)
    weight = (block_ref[0, NEAR + at], block_ref[1, NEAR + at])
    for d in range(1, FAR):
        for s in range(batch):
            factor = spread(after[s : s + 1])
            for part in range(2):
                lines_ref[part, d - 1, s] = factor * weight[part]
        if d < FAR - 1:
            after = after * back[d - 1]
            weight = times(weight, (small_ref[1], small_ref[2]))


def third(batch, length, local_ref, decay_ref, inside_ref, lines_ref, *rest):
    far_refs, (y_hbm, y_ref, sems) = rest[: len(SENDS)], rest[len(SENDS) :]
    run = lax.axis_index("seq") // NEAR
    flip = sign()
    size = length // 2
    stores = []
    for s in range(batch):
        terms = []
        for sends, far_ref in zip(SENDS, reversed(far_refs)):
            d = sum(jnp.where(run == to, to - at - 1, 0) for at, to, _ in sends)
            terms.append((lines_ref[0, d, s], lines_ref[1, d, s], far_ref[s]))
        carry = inside_ref[s] + gathered(terms, flip)
        turned = flip * swapped(carry)
        for half in range(2):
            for t in range(half * size, half * size + size):
                state = local_ref[s, t] + (decay_ref[0, s, t] * carry + decay_ref[1, s, t] * turned)
                y_ref[pl.ds((s * length + t) * ROWS, ROWS)] = state.astype(jnp.bfloat16)
            rows = pl.ds((2 * s + half) * size * ROWS, size * ROWS)
            store = pltpu.make_async_copy(y_ref.at[rows], y_hbm.at[rows], sems.at[2 * s + half])
            store.start()
            stores.append(store)
    for store in stores:
        store.wait()


def shards(inputs, decay_rate, phase, keep):
    batch, length, parts, width = inputs.shape
    tiles = width // LANES
    blocks = keep.shape[1] // length
    chunks = length // STEP
    f32 = functools.partial(jax.ShapeDtypeStruct, dtype=jnp.float32)
    tile = (ROWS, LANES)
    total = batch * length * ROWS
    x = inputs.reshape(batch, length, parts, tiles, LANES).transpose(0, 1, 3, 2, 4).reshape(total, LANES)
    kept = keep.reshape(batch, blocks, length).transpose(1, 0, 2)
    given = (x, decay_rate.reshape(tiles, LANES), phase.reshape(tiles, LANES), kept)
    x, send, ends, step, chunk, block, small, ended, kepts, totals, products, keeps = pl.pallas_call(
        functools.partial(first, batch, length),
        out_shape=[
            jax.ShapeDtypeStruct((total, LANES), jnp.bfloat16),
            f32((NEAR, batch, *tile)),
            f32((batch, chunks, 2, *tile)),
            f32((2, STEP, *tile)),
            f32((2, chunks, *tile)),
            f32((2, 2 * NEAR, *tile)),
            f32((3, *tile)),
            f32((batch * chunks, LANES)),
            f32((batch, length, LANES)),
            f32((2, NEAR, batch, *tile)),
            f32((NEAR, batch, LANES)),
            f32((blocks, batch, LANES)),
        ],
        in_specs=[HBM] * 4,
        out_specs=[VMEM] * 12,
        scratch_shapes=[
            pltpu.VMEM((2, tiles, LANES), jnp.float32),
            pltpu.VMEM((ROWS, LANES), jnp.float32),
            pltpu.SemaphoreType.DMA((4 + batch,)),
        ],
        compiler_params=LIMIT,
    )(*(pltpu.with_memory_space_constraint(value, pltpu.HBM) for value in given))

    runs = range(blocks // NEAR)
    near = lax.all_to_all(
        send.reshape(NEAR, batch * ROWS, LANES),
        "seq",
        0,
        0,
        axis_index_groups=[[run * NEAR + m for m in range(NEAR)] for run in runs],
        tiled=True,
    ).reshape(send.shape)
    sums = pl.pallas_call(
        functools.partial(second, batch),
        out_shape=f32((batch, *tile)),
        in_specs=[VMEM] * 2,
        out_specs=VMEM,
        compiler_params=LIMIT,
    )(near, totals)
    flat = sums.reshape(batch * ROWS, LANES)
    far = []
    for sends in SENDS:
        pairs = [
            (at * NEAR + m, to * NEAR + ((m + cross * WIDE) % NEAR ^ 1)) for at, to, cross in sends for m in range(NEAR)
        ]
        far.append(lax.ppermute(flat, "seq", pairs).reshape(sums.shape))
    local, decay, inside, lines = pl.pallas_call(
        functools.partial(middle, batch, length),
        out_shape=[
            f32((batch, length, *tile)),
            f32((2, batch, length, *tile)),
            f32((batch, *tile)),
            f32((2, FAR - 1, batch, *tile)),
        ],
        in_specs=[VMEM] * 11,
        out_specs=[VMEM] * 4,
        compiler_params=LIMIT,
        cost_estimate=pl.CostEstimate(flops=10_000_000, bytes_accessed=6_000_000, transcendentals=0),
    )(x, near, ends, step, chunk, block, small, ended, kepts, products, keeps)
    y = pl.pallas_call(
        functools.partial(third, batch, length),
        out_shape=jax.ShapeDtypeStruct((total, LANES), jnp.bfloat16),
        in_specs=[VMEM] * (4 + len(SENDS)),
        out_specs=HBM,
        scratch_shapes=[
            pltpu.VMEM((total, LANES), jnp.bfloat16),
            pltpu.SemaphoreType.DMA((2 * batch,)),
        ],
        compiler_params=LIMIT,
    )(local, decay, inside, lines, *reversed(far))
    y = y.reshape(batch, length, tiles, parts, LANES).transpose(0, 1, 3, 2, 4)
    return y.reshape(inputs.shape)


def solution(mesh):
    split = Mesh(mesh.devices, ("chan", "seq"))
    return jax.shard_map(
        shards,
        mesh=split,
        in_specs=(P(None, "seq", None, "chan"), P("chan"), P("chan"), P()),
        out_specs=P(None, "seq", None, "chan"),
        check_vma=False,
    )
```

```python
import functools

import jax
import jax.numpy as jnp
from jax import lax
from jax.experimental import pallas as pl
from jax.experimental.pallas import tpu as pltpu
from jax.sharding import Mesh
from jax.sharding import PartitionSpec as P

LANES = 128
ROWS = 8
STEP = 16
NEAR = 16
FAR = 4
WIDE = 8
SENDS = (
    ((0, 1, 0),),
    ((0, 3, 0),),
    ((0, 2, 1), (1, 3, 1)),
    ((1, 2, 0), (2, 3, 0)),
)

HBM = pl.BlockSpec(memory_space=pltpu.HBM)
VMEM = pl.BlockSpec(memory_space=pltpu.VMEM)
LIMIT = pltpu.CompilerParams(vmem_limit_bytes=8 * 1024 * 1024)


def times(one, two):
    a, b = one
    c, d = two
    return (a * c - b * d, a * d + b * c)


def powers(base, count):
    found = [None, base]
    for n in range(2, count):
        found.append(times(found[n // 2], found[n - n // 2]))
    return found


def places():
    return lax.broadcasted_iota(jnp.int32, (ROWS, LANES), 0)


def sign():
    return jnp.where(places() % 2 == 0, -1.0, 1.0)


def swapped(value):
    return jnp.take_along_axis(value, places() ^ 1, axis=0, mode="promise_in_bounds")


def spread(row):
    return jnp.broadcast_to(row, (ROWS, LANES))


def doubled(rows):
    return jnp.concatenate([rows[j // 2 : j // 2 + 1] for j in range(ROWS)], axis=0)


TURNS = ((1, 4), (4, 4), (16, 4), (64, 2))


def turned_product(value, width, turns):
    rolled = [value] + [pltpu.roll(value, width * n, 1) for n in range(1, turns)]
    while len(rolled) > 1:
        rolled = [rolled[n] * rolled[n + 1] for n in range(0, len(rolled), 2)]
    return rolled[0]


def lane_product(value):
    for width, turns in TURNS:
        value = turned_product(value, width, turns)
    return value


def windows(value):
    for width, turns in TURNS[:2]:
        value = turned_product(value, width, turns)
    return value


def minus_expm1_twice(rate):
    u = 2.0 * rate
    series = u * (1.0 - u / 2 * (1.0 - u / 3 * (1.0 - u / 4 * (1.0 - u / 5 * (1.0 - u / 6)))))
    return jnp.where(u < 0.1, series, 1.0 - jnp.exp(-u))


def first(batch, length, x_hbm, rate_hbm, phase_hbm, keep_hbm, x_ref, send_ref, ends_ref, step_ref, chunk_ref, block_ref,
          small_ref, ended_ref, kept_ref, total_ref, near_ref, keep_ref, param_ref, own_ref, sems):
    me = lax.axis_index("seq")
    run = me // NEAR
    chunks = length // STEP
    span = length * ROWS
    pieces = [
        pltpu.make_async_copy(x_hbm.at[pl.ds(s * span, span)], x_ref.at[pl.ds(s * span, span)], sems.at[4 + s])
        for s in range(batch)
    ]
    loads = [
        pltpu.make_async_copy(rate_hbm, param_ref.at[0], sems.at[0]),
        pltpu.make_async_copy(phase_hbm, param_ref.at[1], sems.at[1]),
        pltpu.make_async_copy(keep_hbm.at[me], own_ref.at[pl.ds(0, batch)], sems.at[2]),
        pltpu.make_async_copy(keep_hbm, keep_ref, sems.at[3]),
    ]
    own_ref[...] = jnp.ones_like(own_ref)
    for load in loads[:3] + pieces[:1] + loads[3:] + pieces[1:]:
        load.start()
    flip = sign()
    loads[0].wait()
    loads[1].wait()
    loads[2].wait()
    own = own_ref[...]
    upright = jnp.transpose(own)
    for s in range(batch):
        for t in range(0, length, ROWS):
            kept_ref[s, pl.ds(t, ROWS)] = jnp.broadcast_to(upright[t : t + ROWS, s : s + 1], (ROWS, LANES))
    ended = windows(own)
    rate, phase = doubled(param_ref[0]), doubled(param_ref[1])
    magnitude = jnp.exp(-rate)
    one, zero = jnp.ones_like(rate), jnp.zeros_like(rate)
    lam = (magnitude * jnp.cos(phase), magnitude * jnp.sin(phase))
    gamma = jnp.sqrt(minus_expm1_twice(rate))
    step = powers(lam, STEP + 1)
    chunk = powers(step[STEP], chunks + 1)
    block = powers(chunk[chunks], NEAR + 1)
    small_ref[0] = gamma
    for part in range(2):
        small_ref[1 + part] = block[NEAR][part]
        for n in range(STEP):
            step_ref[part, n] = step[n + 1][part]
        chunk_ref[part, 0] = zero if part else one
        for n in range(1, chunks):
            chunk_ref[part, n] = chunk[n][part]
        for n in range(NEAR):
            block_ref[part, n] = zero
        block_ref[part, NEAR] = zero if part else one
        for n in range(1, NEAR):
            block_ref[part, NEAR + n] = block[n][part]

    def ends(s):
        direct, cross = [None] * chunks, [None] * chunks
        for i in range(STEP):
            n = STEP - 1 - i
            for k in range(chunks):
                t = k * STEP + i
                x = x_ref[pl.ds(s * span + t * ROWS, ROWS)].astype(jnp.float32)
                if i == 0:
                    direct[k], cross[k] = step[n][0] * x, step[n][1] * x
                    continue
                kept = spread(kept_ref[s, pl.ds(t, 1)])
                direct[k] = kept * direct[k] + (step[n][0] * x if n else x)
                cross[k] = kept * cross[k] + step[n][1] * x if n else kept * cross[k]
        one_way = other = None
        for k in range(chunks):
            ends_ref[s, k, 0], ends_ref[s, k, 1] = direct[k], cross[k]
            last = k * STEP + STEP - 1
            decay = jnp.broadcast_to(ended[s : s + 1, last : last + 1], (ROWS, LANES))
            ended_ref[pl.ds(s * chunks + k, 1)] = decay[:1]
            if k < chunks - 1:
                n = chunks - 1 - k
                real = chunk[n][0] * direct[k] - chunk[n][1] * cross[k]
                imag = chunk[n][0] * cross[k] + chunk[n][1] * direct[k]
            else:
                real, imag = direct[k], cross[k]
            one_way, other = (real, imag) if k == 0 else (decay * one_way + real, decay * other + imag)
        state = gamma * (one_way + flip * swapped(other))
        for n in range(NEAR):
            send_ref[n, s] = state

    def weights(near):
        after = jnp.ones((batch, LANES), jnp.float32)
        for m in reversed(range(NEAR)):
            near_ref[m] = near[m]
            for s in range(batch):
                factor = spread(after[s : s + 1])
                for part in range(2):
                    total_ref[part, m, s] = factor * block_ref[part, 2 * NEAR - 1 - m]
            after = after * near[m]

    pieces[0].wait()
    ends(0)
    loads[3].wait()
    pieces[1].wait()
    near = [keep_ref[run * NEAR + m] for m in range(NEAR)]
    for width, turns in TURNS[:2]:
        near = [turned_product(value, width, turns) for value in near]
    ends(1)
    pieces[2].wait()
    for width, turns in TURNS[2:]:
        near = [turned_product(value, width, turns) for value in near]
    weights(near)
    ends(2)


def gathered(terms, flip):
    direct = cross = None
    for real, imag, x in terms:
        one, two = real * x, imag * x
        direct, cross = (one, two) if direct is None else (direct + one, cross + two)
    return direct + flip * swapped(cross)


def second(batch, got_ref, total_ref, send_ref):
    flip = sign()
    for s in range(batch):
        send_ref[s] = gathered([(total_ref[0, m, s], total_ref[1, m, s], got_ref[m, s]) for m in range(NEAR)], flip)


def middle(batch, length, x_ref, got_ref, ends_ref, step_ref, chunk_ref, block_ref, small_ref, ended_ref, kept_ref,
           near_ref, keep_ref, local_ref, decay_ref, reach_ref, inside_ref, lines_ref):
    me = lax.axis_index("seq")
    run, at = me // NEAR, me % NEAR
    chunks = length // STEP
    span = length * ROWS
    flip = sign()
    products = []
    for n in range(FAR):
        product = keep_ref[n * NEAR]
        for m in range(1, NEAR):
            product = product * keep_ref[n * NEAR + m]
        products.append(product)
    back = []
    for d in range(1, FAR - 1):
        before = products[0]
        for m in range(1, FAR):
            before = jnp.where(run - d == m, products[m], before)
        back.append(lane_product(before))

    gamma = small_ref[0]
    lam_re, lam_im = step_ref[0, 0], step_ref[1, 0] * flip
    jump_re, jump_im = step_ref[0, STEP - 1], step_ref[1, STEP - 1] * flip
    state, reach = {}, {}
    for s in range(batch):
        for k in range(chunks):
            if k == 0:
                state[s, k], reach[s, k] = jnp.zeros_like(gamma), jnp.ones_like(gamma)
                continue
            h = state[s, k - 1]
            decay = spread(ended_ref[pl.ds(s * chunks + k - 1, 1)])
            end = gamma * (ends_ref[s, k - 1, 0] + flip * swapped(ends_ref[s, k - 1, 1]))
            state[s, k] = decay * (jump_re * h + jump_im * swapped(h)) + end
            reach[s, k] = decay * reach[s, k - 1]
    for k in range(chunks):
        for i in range(STEP):
            t = k * STEP + i
            power = times((step_ref[0, i], step_ref[1, i]), (chunk_ref[0, k], chunk_ref[1, k]))
            for s in range(batch):
                kept = spread(kept_ref[s, pl.ds(t, 1)])
                x = gamma * x_ref[pl.ds(s * span + t * ROWS, ROWS)].astype(jnp.float32)
                h = state[s, k]
                state[s, k] = kept * (lam_re * h + lam_im * swapped(h)) + x
                reach[s, k] = kept * reach[s, k]
                local_ref[s, t] = state[s, k]
                reach_ref[s, pl.ds(t, 1)] = reach[s, k][:1]
            for part in range(2):
                decay_ref[part, t] = power[part]

    after = jnp.ones((batch, LANES), jnp.float32)
    terms = [[] for _ in range(batch)]
    for m in reversed(range(NEAR)):
        real, imag = block_ref[0, NEAR - 1 + at - m], block_ref[1, NEAR - 1 + at - m]
        for s in range(batch):
            factor = spread(after[s : s + 1])
            terms[s].append((factor * real, factor * imag, got_ref[m, s]))
        after = after * jnp.where(m < at, near_ref[m], 1.0)
    for s in range(batch):
        inside_ref[s] = gathered(terms[s], flip)
    weight = (block_ref[0, NEAR + at], block_ref[1, NEAR + at])
    for d in range(1, FAR):
        for s in range(batch):
            factor = spread(after[s : s + 1])
            for part in range(2):
                lines_ref[part, d - 1, s] = factor * weight[part]
        if d < FAR - 1:
            after = after * back[d - 1]
            weight = times(weight, (small_ref[1], small_ref[2]))


def third(batch, length, local_ref, decay_ref, reach_ref, inside_ref, lines_ref, *rest):
    far_refs, (y_hbm, y_ref, sems) = rest[: len(SENDS)], rest[len(SENDS) :]
    run = lax.axis_index("seq") // NEAR
    flip = sign()
    size = length // 2
    stores = []
    for s in range(batch):
        terms = []
        for sends, far_ref in zip(SENDS, reversed(far_refs)):
            d = sum(jnp.where(run == to, to - at - 1, 0) for at, to, _ in sends)
            terms.append((lines_ref[0, d, s], lines_ref[1, d, s], far_ref[s]))
        carry = inside_ref[s] + gathered(terms, flip)
        turned = flip * swapped(carry)
        for half in range(2):
            for t in range(half * size, half * size + size):
                kept = spread(reach_ref[s, pl.ds(t, 1)])
                state = local_ref[s, t] + kept * (decay_ref[0, t] * carry + decay_ref[1, t] * turned)
                y_ref[pl.ds((s * length + t) * ROWS, ROWS)] = state.astype(jnp.bfloat16)
            rows = pl.ds((2 * s + half) * size * ROWS, size * ROWS)
            store = pltpu.make_async_copy(y_ref.at[rows], y_hbm.at[rows], sems.at[2 * s + half])
            store.start()
            stores.append(store)
    for store in stores:
        store.wait()


def shards(inputs, decay_rate, phase, keep):
    batch, length, parts, width = inputs.shape
    tiles = width // LANES
    blocks = keep.shape[1] // length
    chunks = length // STEP
    f32 = functools.partial(jax.ShapeDtypeStruct, dtype=jnp.float32)
    tile = (ROWS, LANES)
    total = batch * length * ROWS
    x = inputs.reshape(batch, length, parts, tiles, LANES).transpose(0, 1, 3, 2, 4).reshape(total, LANES)
    kept = keep.reshape(batch, blocks, length).transpose(1, 0, 2)
    given = (x, decay_rate.reshape(tiles, LANES), phase.reshape(tiles, LANES), kept)
    x, send, ends, step, chunk, block, small, ended, kepts, totals, products, keeps = pl.pallas_call(
        functools.partial(first, batch, length),
        out_shape=[
            jax.ShapeDtypeStruct((total, LANES), jnp.bfloat16),
            f32((NEAR, batch, *tile)),
            f32((batch, chunks, 2, *tile)),
            f32((2, STEP, *tile)),
            f32((2, chunks, *tile)),
            f32((2, 2 * NEAR, *tile)),
            f32((3, *tile)),
            f32((batch * chunks, LANES)),
            f32((batch, length, LANES)),
            f32((2, NEAR, batch, *tile)),
            f32((NEAR, batch, LANES)),
            f32((blocks, batch, LANES)),
        ],
        in_specs=[HBM] * 4,
        out_specs=[VMEM] * 12,
        scratch_shapes=[
            pltpu.VMEM((2, tiles, LANES), jnp.float32),
            pltpu.VMEM((ROWS, LANES), jnp.float32),
            pltpu.SemaphoreType.DMA((4 + batch,)),
        ],
        compiler_params=LIMIT,
    )(*(pltpu.with_memory_space_constraint(value, pltpu.HBM) for value in given))

    runs = range(blocks // NEAR)
    near = lax.all_to_all(
        send.reshape(NEAR, batch * ROWS, LANES),
        "seq",
        0,
        0,
        axis_index_groups=[[run * NEAR + m for m in range(NEAR)] for run in runs],
        tiled=True,
    ).reshape(send.shape)
    sums = pl.pallas_call(
        functools.partial(second, batch),
        out_shape=f32((batch, *tile)),
        in_specs=[VMEM] * 2,
        out_specs=VMEM,
        compiler_params=LIMIT,
    )(near, totals)
    flat = sums.reshape(batch * ROWS, LANES)
    far = []
    for sends in SENDS:
        pairs = [
            (at * NEAR + m, to * NEAR + ((m + cross * WIDE) % NEAR ^ 1)) for at, to, cross in sends for m in range(NEAR)
        ]
        far.append(lax.ppermute(flat, "seq", pairs).reshape(sums.shape))
    local, decay, reach, inside, lines = pl.pallas_call(
        functools.partial(middle, batch, length),
        out_shape=[
            f32((batch, length, *tile)),
            f32((2, length, *tile)),
            f32((batch, length, LANES)),
            f32((batch, *tile)),
            f32((2, FAR - 1, batch, *tile)),
        ],
        in_specs=[VMEM] * 11,
        out_specs=[VMEM] * 5,
        compiler_params=LIMIT,
        cost_estimate=pl.CostEstimate(flops=10_000_000, bytes_accessed=6_000_000, transcendentals=0),
    )(x, near, ends, step, chunk, block, small, ended, kepts, products, keeps)
    y = pl.pallas_call(
        functools.partial(third, batch, length),
        out_shape=jax.ShapeDtypeStruct((total, LANES), jnp.bfloat16),
        in_specs=[VMEM] * (5 + len(SENDS)),
        out_specs=HBM,
        scratch_shapes=[
            pltpu.VMEM((total, LANES), jnp.bfloat16),
            pltpu.SemaphoreType.DMA((2 * batch,)),
        ],
        compiler_params=LIMIT,
    )(local, decay, reach, inside, lines, *reversed(far))
    y = y.reshape(batch, length, tiles, parts, LANES).transpose(0, 1, 3, 2, 4)
    return y.reshape(inputs.shape)


def solution(mesh):
    split = Mesh(mesh.devices, ("chan", "seq"))
    return jax.shard_map(
        shards,
        mesh=split,
        in_specs=(P(None, "seq", None, "chan"), P("chan"), P("chan"), P()),
        out_specs=P(None, "seq", None, "chan"),
        check_vma=False,
    )
```
